32 devices in a mesh: dp: 8 (over z, x), mp: 4 (over y, core).
Axes of the slice: x: 2, y: 2, z: 4, core: 2. Of those that a mesh axis runs over, the one named last changes fastest.
Arguments:
- vision_rows: bfloat16 [1024, 1024], P('dp'), may hold values from -6 to 6
- image_count: int32 [32], P('dp'), may hold values from 0 to 4
- proj_flat: bfloat16 [32768, 128], P(('dp', 'mp')), may hold values from -0.1875 to 0.1875
- text_embeds: bfloat16 [3072, 4096], P(('dp', 'mp')), may hold values from -6 to 6
- norm_gain: float32 [4096], replicated, may hold values from 0.1 to 1.9
- q_weight: bfloat16 [4096, 4096], P(None, 'mp'), may hold values from -0.09375 to 0.09375
- q_grad: bfloat16 [4096, 4096], P('dp', 'mp'), may hold values from -6 to 6
Outputs:
- text_grad: bfloat16 [3072, 4096], P(('dp', 'mp'))
- proj_grad: float32 [32768, 128], P(('dp', 'mp'))
The draws below stay inside these ranges and needn't reach their ends.
Inputs may be any that keep to these rules, and one draw needn't show every extreme that they name: Slot s of device k holds an image when s < image_count[k]; other slots are padding.
All inputs are finite; a program needn't handle non-finite values.
Results may differ from the reference program's by a relative error of at most 0.014.
Values may be sent and summed in bfloat16 or wider, within the bound.
A program may use at most 64 MiB of HBM per device.

```python
import jax
import jax.numpy as jnp
from jax import lax

D = 4096
ENC = 1024
IMG_MAX = 4
PATCH = 8
TEXT_DEV = 96
IMG_ROWS = 32
ROWS_DEV = 128
PROJ_ROWS = 1024
N_DP = 8
N_MP = 4


def plant(drawn, own_key, least, largest):
    longest = drawn.shape.index(max(drawn.shape))
    spots = []
    for shift in (0, 1):
        where = [jax.random.randint(jax.random.fold_in(own_key, axis), (), 0, length) for axis, length in enumerate(drawn.shape)]
        where[longest] = (where[longest] + shift) % drawn.shape[longest]
        spots.append(tuple(where))
    return drawn.at[spots[0]].set(least).at[spots[1]].set(largest)


def block_scale(key, extent, cuts, smallest, high):
    level = 1.0
    for position, blocks in cuts:
        heights = jax.random.uniform(jax.random.fold_in(jax.random.fold_in(key, 6), position), (blocks,), jnp.float32, smallest / len(cuts), high / len(cuts))
        level = level * jnp.repeat(jnp.exp(heights), extent[position] // blocks).reshape((-1,) + (1,) * (len(extent) - 1 - position))
    return level


def bell_draw(own_key, dims, deviation, most, split=(), kind=jnp.bfloat16):
    gain = block_scale(own_key, dims, split, -0.22, 0.18) if split else 1.0
    array = jax.random.normal(own_key, dims, jnp.float32) * deviation * gain
    return jnp.minimum(jnp.maximum(array, -most), most).astype(kind)


def setup_inputs(seed: int = 0) -> dict:
    streams_of = jax.random.split(jax.random.key(seed), 8)
    vision_rows = bell_draw(streams_of[0], (N_DP * N_MP * IMG_ROWS, ENC), 1.0, 6.0, ((0, 8),))
    image_count = plant(jax.random.randint(streams_of[1], (N_DP * N_MP,), 0, IMG_MAX + 1), jax.random.fold_in(streams_of[1], 1), 0, IMG_MAX).astype(jnp.int32)
    proj_flat = bell_draw(streams_of[2], (N_DP * N_MP * PROJ_ROWS, 128), ENC ** -0.5, 0.1875, ((0, 32),))
    text_embeds = bell_draw(streams_of[3], (N_DP * N_MP * TEXT_DEV, D), 1.0, 6.0, ((0, 32),))
    norm_gain = jnp.clip(1.0 + 0.18 * jax.random.normal(streams_of[4], (D,), jnp.float32), 0.1, 1.9)
    q_weight = bell_draw(streams_of[5], (D, D), D ** -0.5, 0.09375, ((1, 4),))
    q_grad = bell_draw(streams_of[6], (N_DP * N_MP * ROWS_DEV, D), 1.0, 6.0, ((0, 8), (1, 4)))
    return {"vision_rows": vision_rows, "image_count": image_count, "proj_flat": proj_flat, "text_embeds": text_embeds, "norm_gain": norm_gain, "q_weight": q_weight, "q_grad": q_grad}


norm_eps = 1e-05

def reference(vision_rows, image_count, proj_flat, text_embeds, norm_gain, q_weight, q_grad):
    block_cols = D // N_MP
    used_count = ENC * block_cols
    stored = proj_flat.reshape(N_DP, N_MP, PROJ_ROWS * 128).transpose(1, 0, 2)
    stored = stored.reshape(N_MP, N_DP * PROJ_ROWS * 128)[:, :used_count]
    proj_weight = stored.reshape(N_MP, ENC, block_cols).transpose(1, 0, 2).reshape(ENC, D)
    image_embed = jnp.dot(vision_rows, proj_weight, preferred_element_type=jnp.float32).astype(jnp.bfloat16)
    image_blocks = image_embed.reshape(N_DP * N_MP, IMG_ROWS, D)
    text_blocks = text_embeds.reshape(N_DP * N_MP, TEXT_DEV, D)
    decoder_in = jnp.concatenate([image_blocks, text_blocks], axis=1).reshape(-1, D)
    inputs = decoder_in.astype(jnp.float32)
    inv_rms = lax.rsqrt(lax.optimization_barrier(jnp.mean(inputs * inputs, axis=-1, keepdims=True)) + norm_eps)
    norm_grad = jnp.zeros(inputs.shape, jnp.float32)
    for member in range(N_MP):
        left = q_grad[:, member * block_cols:(member + 1) * block_cols]
        right = q_weight[:, member * block_cols:(member + 1) * block_cols]
        term = jnp.dot(left, right.T, preferred_element_type=jnp.float32).astype(jnp.bfloat16)
        term = lax.optimization_barrier(term)
        norm_grad = norm_grad + term.astype(jnp.float32)
    scaled = norm_gain[None, :] * norm_grad
    inner_mean = lax.optimization_barrier(jnp.mean(scaled * inputs, axis=-1, keepdims=True))
    input_grad = inv_rms * scaled - inputs * inv_rms ** 3 * inner_mean
    grad_blocks = input_grad.reshape(N_DP * N_MP, ROWS_DEV, D)
    text_grad = grad_blocks[:, IMG_ROWS:, :].reshape(-1, D).astype(jnp.bfloat16)
    live_slots = jnp.arange(IMG_MAX, dtype=jnp.int32)[None, :] < image_count[:, None]
    live_rows = jnp.repeat(live_slots, PATCH, axis=1)
    image_grad = jnp.where(live_rows[:, :, None], grad_blocks[:, :IMG_ROWS, :], 0.0)
    image_grad = image_grad.reshape(-1, D).astype(jnp.bfloat16)
    grad_scale = 1.0 / jnp.sqrt(jnp.float32(N_DP * N_MP * IMG_ROWS))
    proj_full = jnp.dot(vision_rows.T, image_grad, preferred_element_type=jnp.float32) * grad_scale
    flat_blocks = proj_full.reshape(ENC, N_MP, block_cols).transpose(1, 0, 2).reshape(N_MP, used_count)
    flat_blocks = jnp.pad(flat_blocks, ((0, 0), (0, N_DP * PROJ_ROWS * 128 - used_count)))
    proj_grad = flat_blocks.reshape(N_MP, N_DP, PROJ_ROWS * 128).transpose(1, 0, 2)
    proj_grad = proj_grad.reshape(N_DP * N_MP * PROJ_ROWS, 128)
    return (text_grad, proj_grad)
```

```python
import functools

import jax
import jax.numpy as jnp
from jax import lax
from jax.experimental import pallas as pl
from jax.experimental.pallas import tpu as pltpu
from jax.sharding import PartitionSpec as P

IMG_MAX = 4
PATCH = 8
ROWS_DEV = 128
CORES = 2
SIDE = 2
CHUNKS = 4
PIECES = 2
LANES = 128
TILE = 256
ROW_STEP = 16

MESH = pl.DeviceIdType.MESH

norm_eps = 1e-05


def row_term(left, weight):
    return lax.dot_general(
        left, weight, (((1,), (1,)), ((), ())), preferred_element_type=jnp.float32
    )


def remote(src, dst, send, recv, device):
    return pltpu.make_async_remote_copy(
        src_ref=src, dst_ref=dst, send_sem=send, recv_sem=recv,
        device_id=device, device_id_type=MESH,
    )


class VisionGather:
    def __init__(self, depth, me, member, buf, block_rows, send, recv, mate_send, mate_recv):
        self.depth, self.me, self.member = depth, me, member
        self.z, self.x = me // SIDE, me % SIDE
        self.core = member % CORES
        self.mate = member + 1 - 2 * self.core
        self.buf, self.block_rows = buf, block_rows
        self.send, self.recv = send, recv
        self.mate_send, self.mate_recv = mate_send, mate_recv
        self.half = block_rows // CORES
        self.step = self.half // CHUNKS

    def place(self, block, chunk, core):
        first = block * self.block_rows + core * self.half + chunk * self.step
        return self.buf.at[pl.ds(pl.multiple_of(first, self.step), self.step)]

    def copy(self, zz, x, chunk, way):
        block = zz * SIDE + x
        place = self.place(block, chunk, self.core)
        target = (self.me + SIDE, self.me - SIDE, self.z * SIDE + 1 - self.x)[way]
        return remote(
            place, place, self.send.at[way, zz, chunk], self.recv.at[block, chunk],
            (target, self.member),
        )

    def to_mate(self, block, chunk):
        place = self.place(block, chunk, self.core)
        return remote(
            place, place, self.mate_send.at[block, chunk], self.mate_recv.at[block, chunk],
            (self.me, self.mate),
        )

    def from_mate(self, block, chunk):
        place = self.place(block, chunk, 1 - self.core)
        return remote(
            place, place, self.mate_send.at[block, chunk], self.mate_recv.at[block, chunk],
            (self.me, self.mate),
        )

    def start(self):
        for chunk in range(CHUNKS):
            @pl.when(self.z < self.depth - 1)
            def _():
                self.copy(self.z, self.x, chunk, 0).start()

            @pl.when(self.z > 0)
            def _():
                self.copy(self.z, self.x, chunk, 1).start()

            self.copy(self.z, self.x, chunk, 2).start()

    def relay(self, hop, chunk):
        below, above = self.z - hop, self.z + hop

        @pl.when(below >= 0)
        def _():
            self.copy(below, self.x, chunk, 0).wait_recv()

            @pl.when(self.z < self.depth - 1)
            def _():
                self.copy(below, self.x, chunk, 0).start()

            self.copy(below, self.x, chunk, 2).start()
            self.to_mate(below * SIDE + self.x, chunk).start()

        @pl.when(above < self.depth)
        def _():
            self.copy(above, self.x, chunk, 1).wait_recv()

            @pl.when(self.z > 0)
            def _():
                self.copy(above, self.x, chunk, 1).start()

            self.copy(above, self.x, chunk, 2).start()
            self.to_mate(above * SIDE + self.x, chunk).start()

    def levels(self, hop, use):
        for zz in (self.z,) if hop == 0 else (self.z - hop, self.z + hop):
            @pl.when((zz >= 0) & (zz < self.depth))
            def _():
                use(zz)

    def side(self, hop, chunk):
        def take(zz):
            self.copy(zz, 1 - self.x, chunk, 2).wait_recv()
            self.to_mate(zz * SIDE + 1 - self.x, chunk).start()

        self.levels(hop, take)

    def arrive(self, zz):
        for chunk in range(CHUNKS):
            @pl.when(zz != self.z)
            def _():
                self.from_mate(zz * SIDE + self.x, chunk).wait_recv()

            self.from_mate(zz * SIDE + 1 - self.x, chunk).wait_recv()

    def drain(self):
        for zz in range(self.depth):
            for chunk in range(CHUNKS):
                @pl.when((self.z >= zz) & (self.z < self.depth - 1))
                def _():
                    self.copy(zz, self.x, chunk, 0).wait_send()

                @pl.when((self.z <= zz) & (self.z > 0))
                def _():
                    self.copy(zz, self.x, chunk, 1).wait_send()

                self.copy(zz, self.x, chunk, 2).wait_send()

                @pl.when(zz != self.z)
                def _():
                    self.to_mate(zz * SIDE + self.x, chunk).wait_send()

                self.to_mate(zz * SIDE + 1 - self.x, chunk).wait_send()


def kernel(
    shards, groups, grad_scale,
    count_ref, proj_hbm, vision_hbm, gain_hbm, q_hbm, w_hbm, text_hbm,
    text_hbm_out, proj_out,
    pv, vv, gain_ref, q_image, q_text, wv, tv, text_out,
    own_text, own_image, mate_text, mate_image, sum_text, sum_image,
    far_text, far_image, w_flat, w_out, wt, n_out, nt, xt, gt, gain_t, o_out, o_in,
    stat_own, stat_near, stat_sum, stat_far,
    p_sem, vis_sem, gain_sem, q_sem, w_sem, t_sem, to_sem,
    v_send, v_recv, vm_send, vm_recv, wt_send, wt_recv, n_send, n_recv, o_send, o_recv,
    mt_send, mt_recv, mi_send, mi_recv, ft_send, ft_recv, fi_send, fi_recv,
    s_send, s_recv, z_send, z_recv,
):
    me, member = lax.axis_index("dp"), lax.axis_index("mp")
    depth = shards // SIDE
    chips = groups // CORES
    y, core = member // CORES, member % CORES
    mate = y * CORES + 1 - core
    z, x = me // SIDE, me % SIDE
    bc = wv.shape[1]
    span = bc // shards
    fold = bc // LANES
    shard_k = wt.shape[1] // shards
    image_rows = q_image.shape[0]
    per_image = image_rows // groups
    text_rows = tv.shape[0]
    rows_dev = per_image + text_rows
    width = groups * bc
    f32, bf16 = jnp.float32, jnp.bfloat16

    far = [lax.rem(y + step, chips) for step in range(1, chips)]
    order = [yy * CORES + lax.rem(core + flip, CORES) for yy in far + [y] for flip in (1, 0)]
    early = len(order) - CORES
    offsets = sorted(range(1, depth), key=lambda o: -min(o, depth - o)) + [0]
    targets = [
        lax.rem(z + o, depth) * SIDE + (x if flip else 1 - x) for o in offsets for flip in (0, 1)
    ]
    levels = [lax.rem(z + o, depth) for o in offsets]
    last = shards - 1

    p_copy = pltpu.make_async_copy(proj_hbm, pv, p_sem)
    p_copy.start()
    own_rows = pl.ds(pl.multiple_of(me * image_rows, image_rows), image_rows)
    vis_copy = pltpu.make_async_copy(vision_hbm, vv.at[own_rows], vis_sem)
    vis_copy.start()
    q_copies = []
    for g in range(groups):
        q_copies.append(pltpu.make_async_copy(
            q_hbm.at[pl.ds(g * rows_dev, per_image)],
            q_image.at[pl.ds(g * per_image, per_image)], q_sem.at[0, g],
        ))
    for g in range(groups):
        q_copies.append(pltpu.make_async_copy(
            q_hbm.at[pl.ds(g * rows_dev + per_image, text_rows)],
            q_text.at[pl.ds(g * text_rows, text_rows)], q_sem.at[1, g],
        ))
    w_copies = [pltpu.make_async_copy(w_hbm.at[j], wv.at[j], w_sem.at[k]) for k, j in enumerate(order)]
    for copy in q_copies[:groups] + w_copies[:1] + q_copies[groups:] + w_copies[1:]:
        copy.start()
    gain_copy = pltpu.make_async_copy(gain_hbm, gain_ref, gain_sem)
    gain_copy.start()
    t_copy = pltpu.make_async_copy(text_hbm, tv, t_sem)
    t_copy.start()

    barrier = pltpu.get_barrier_semaphore()
    across = z * SIDE + 1 - x
    beside = [(me, lax.rem(member + step, groups)) for step in range(1, groups)]
    beside += [(across, lax.rem(member + step, groups)) for step in range(groups)]
    peers = [(lax.rem(me + SIDE * o, shards), member) for o in range(1, depth)]
    peers += [(lax.rem(across + SIDE * o, shards), member) for o in range(1, depth)]
    for device in beside + peers:
        pl.semaphore_signal(barrier, inc=1, device_id=device, device_id_type=MESH)

    p_copy.wait()
    w_flat[...] = pv[...].astype(f32)
    for j in range(shards):
        w_out[j] = w_flat[pl.ds(j, shard_k, stride=fold), :].T.astype(bf16)
    own_k = pl.ds(pl.multiple_of(me * shard_k, shard_k), shard_k)
    wt[:, own_k] = w_out[me]
    vis_copy.wait()

    pl.semaphore_wait(barrier, len(beside) + len(peers))

    vision = VisionGather(depth, me, member, vv, image_rows, v_send, v_recv, vm_send, vm_recv)
    vision.start()

    def w_to(t):
        j = targets[t]
        return remote(w_out.at[j], wt.at[:, own_k], wt_send.at[t], wt_recv.at[me], (j, member))

    def w_from(t):
        j = targets[t]
        cols = pl.ds(pl.multiple_of(j * shard_k, shard_k), shard_k)
        return remote(w_out.at[j], wt.at[:, cols], wt_send.at[t], wt_recv.at[j], (j, member))

    for t in range(last):
        w_to(t).start()

    def text_to_mate(k):
        j = order[k]
        return remote(own_text.at[j, 1 - core], mate_text.at[j], mt_send.at[j], mt_recv.at[j], (me, mate))

    def image_to_mate(yy):
        return remote(
            own_image.at[yy * CORES + 1 - core], mate_image.at[yy],
            mi_send.at[yy], mi_recv.at[yy], (me, mate),
        )

    def text_to_far(k, yy):
        j = order[k]
        return remote(
            sum_text.at[j, yy], far_text.at[y, j], ft_send.at[j, yy], ft_recv.at[y, j],
            (me, yy * CORES + core),
        )

    def text_from_far(k, yy):
        j = order[k]
        return remote(
            sum_text.at[j, yy], far_text.at[yy, j], ft_send.at[j, yy], ft_recv.at[yy, j],
            (me, yy * CORES + core),
        )

    def piece(t):
        return pl.ds(pl.multiple_of(targets[t] * span, span), span)

    def image_to_far(yy, t):
        return remote(
            sum_image.at[yy, piece(t)], far_image.at[y, piece(t)],
            fi_send.at[yy, t], fi_recv.at[y, t], (me, yy * CORES + core),
        )

    def image_from_far(yy, t):
        return remote(
            sum_image.at[yy, piece(t)], far_image.at[yy, piece(t)],
            fi_send.at[yy, t], fi_recv.at[yy, t], (me, yy * CORES + core),
        )

    def image_multiply(k):
        j = order[k]
        w_copies[k].wait()

        @pl.loop(0, bc // TILE)
        def _(n):
            rows = pl.ds(pl.multiple_of(n * TILE, TILE), TILE)
            own_image[j, rows] = row_term(wv[j, rows], q_image[...]).astype(bf16)

        if k % CORES == 0:
            image_to_mate((far + [y])[k // CORES]).start()

    def text_multiply(k):
        j = order[k]

        @pl.loop(0, bc // TILE)
        def _(n):
            cols = pl.ds(pl.multiple_of(n * TILE, TILE), TILE)
            term = row_term(q_text[...], wv[j, cols, :]).astype(bf16)
            for g in range(groups):
                own_text[j, g % CORES, g // CORES, :, cols] = term[g * text_rows : (g + 1) * text_rows]

        text_to_mate(k).start()

    def add_image(yy):
        image_to_mate(yy).wait_recv()
        for t in range(shards):
            rows = piece(t)
            total = own_image[yy * CORES + core, rows].astype(f32) + mate_image[yy, rows].astype(f32)
            sum_image[yy, rows] = total.astype(bf16)
            image_to_far(yy, t).start()

    def add_text(k):
        j = order[k]
        text_to_mate(k).wait_recv()
        for yy in far:
            @pl.loop(0, text_rows // ROW_STEP)
            def _(n):
                rows = pl.ds(pl.multiple_of(n * ROW_STEP, ROW_STEP), ROW_STEP)
                total = own_text[j, core, yy, rows].astype(f32) + mate_text[j, yy, rows].astype(f32)
                sum_text[j, yy, rows] = total.astype(bf16)
            text_to_far(k, yy).start()

    lanes = lax.broadcasted_iota(jnp.int32, (span, image_rows), 1)
    slots = lax.rem(lanes, per_image)
    held = jnp.zeros((span, image_rows), jnp.int32)
    for g in range(groups):
        held = jnp.where(lanes // per_image == g, count_ref[g] * PATCH, held)
    live = slots < held

    def n_to(t):
        j = targets[t]
        return remote(n_out.at[t], nt.at[:, own_lanes], n_send.at[t], n_recv.at[me], (j, member))

    def n_from(t):
        j = targets[t]
        cols = pl.ds(pl.multiple_of(j * image_rows, image_rows), image_rows)
        return remote(n_out.at[t], nt.at[:, cols], n_send.at[t], n_recv.at[j], (j, member))

    own_lanes = pl.ds(pl.multiple_of(me * image_rows, image_rows), image_rows)

    def spread_image(t):
        if t == 0:
            image_to_mate(y).wait_recv()
        for yy in far:
            image_from_far(yy, t).wait_recv()
        rows = piece(t)
        total = own_image[member, rows].astype(f32) + mate_image[y, rows].astype(f32)
        for yy in far:
            total = total + far_image[yy, rows].astype(f32)
        total = jnp.where(live, total, 0.0).astype(bf16)
        if t < last:
            n_out[t] = total
            n_to(t).start()
        else:
            nt[:, own_lanes] = total

    for copy in q_copies[:groups]:
        copy.wait()
    for k in range(len(order)):
        image_multiply(k)
        if k % CORES == 0 and k >= CORES:
            add_image(far[k // CORES - 1])
    for copy in q_copies[groups:]:
        copy.wait()

    pending = []
    for hop in range(1, depth):
        for chunk in range(CHUNKS):
            pending.append(functools.partial(vision.relay, hop, chunk))
        for chunk in range(CHUNKS):
            pending.append(functools.partial(vision.side, hop - 1, chunk))
    for chunk in range(CHUNKS):
        pending.append(functools.partial(vision.side, depth - 1, chunk))
    images = [functools.partial(spread_image, t) for t in range(shards)]

    def step(queue, count):
        for _ in range(min(count, len(queue))):
            queue.pop(0)()

    text_multiply(0)
    step(pending, 1)
    text_multiply(1)
    step(pending, 7)
    for k in range(2, len(order)):
        add_text(k - 2)
        text_multiply(k)
        step(images, 1)
    for k in range(len(order) - 2, len(order)):
        add_text(k)
        step(images, 1)
        step(pending, 4)
    while images or pending:
        step(images, 1)
        step(pending, 2)

    gain_copy.wait()
    own_gain = gain_ref[:, pl.ds(pl.multiple_of(member * bc + me * span, span), span)]
    gain_t[...] = jnp.broadcast_to(own_gain, (image_rows, span)).T

    for t in range(last):
        w_from(t).wait_recv()

    def embed(zz):
        vision.arrive(zz)
        pair = pl.ds(pl.multiple_of(zz * SIDE * image_rows, SIDE * image_rows), SIDE * image_rows)
        rounded = row_term(wt[...], vv[pair]).astype(bf16)
        xt[:, pair] = rounded
        value = rounded.astype(f32)
        squares = jnp.sum(value * value, axis=0, keepdims=True)
        for s in range(SIDE):
            stat_own[pl.ds(zz * SIDE + s, 1)] = squares[:, s * image_rows : (s + 1) * image_rows]

    for hop in range(depth):
        vision.levels(hop, embed)

    for t in reversed(range(shards)):
        if t < last:
            n_from(t).wait_recv()
        j = targets[t]
        cols = pl.ds(pl.multiple_of(j * image_rows, image_rows), image_rows)
        scaled = gain_t[...] * nt[:, cols].astype(f32)
        inner = jnp.sum(scaled * xt[:, cols].astype(f32), axis=0, keepdims=True)
        stat_own[pl.ds(shards + j, 1)] = inner

    def stat_to(k):
        device = beside[k]
        mine = lax.rem(me, SIDE) * groups + member
        return remote(stat_own, stat_near.at[mine], s_send.at[k], s_recv.at[mine], device)

    def stat_from(k):
        device = beside[k]
        theirs = lax.rem(device[0], SIDE) * groups + device[1]
        return remote(stat_own, stat_near.at[theirs], s_send.at[k], s_recv.at[theirs], device)

    for k in range(len(beside)):
        stat_to(k).start()
    total = stat_own[...]
    for k in range(len(beside)):
        stat_from(k).wait_recv()
        total = total + stat_near[lax.rem(beside[k][0], SIDE) * groups + beside[k][1]]
    stat_sum[...] = total

    def line_to(o):
        target = lax.rem(z + o, depth)
        return remote(
            stat_sum, stat_far.at[z], z_send.at[o], z_recv.at[z], (target * SIDE + x, member)
        )

    def line_from(o):
        source = lax.rem(z + o, depth)
        return remote(
            stat_sum, stat_far.at[source], z_send.at[o], z_recv.at[source], (source * SIDE + x, member)
        )

    for o in range(1, depth):
        line_to(o).start()
    for o in range(1, depth):
        line_from(o).wait_recv()
        total = total + stat_far[lax.rem(z + o, depth)]

    inv_all = lax.rsqrt(total[:shards] / width + norm_eps)
    pull_all = inv_all**3 * (total[shards:] / width)
    for b in range(shards):
        cols = pl.ds(b * image_rows, image_rows)
        scaled = gain_t[...] * nt[:, cols].astype(f32)
        grad = inv_all[b : b + 1] * scaled - xt[:, cols].astype(f32) * pull_all[b : b + 1]
        gt[:, cols] = grad.astype(bf16)

    def o_to(t):
        j = targets[t]
        return remote(o_out.at[j], o_in.at[me], o_send.at[t], o_recv.at[me], (j, member))

    def o_from(t):
        j = targets[t]
        return remote(o_out.at[j], o_in.at[j], o_send.at[t], o_recv.at[j], (j, member))

    for i, zz in enumerate(levels):
        cols = pl.ds(pl.multiple_of(zz * SIDE * shard_k, SIDE * shard_k), SIDE * shard_k)
        out = jnp.dot(gt[...], vv[:, cols], preferred_element_type=f32) * grad_scale
        out = out.astype(bf16)
        for s in range(SIDE):
            o_out[zz * SIDE + s] = out[:, s * shard_k : (s + 1) * shard_k]
        for t in range(SIDE * i, SIDE * i + SIDE):
            if t < last:
                o_to(t).start()

    for k in range(len(order)):
        for yy in far:
            text_from_far(k, yy).wait_recv()
    t_copy.wait()

    @pl.loop(0, text_rows // ROW_STEP)
    def _(n):
        rows = pl.ds(pl.multiple_of(n * ROW_STEP, ROW_STEP), ROW_STEP)
        squares = jnp.zeros((ROW_STEP, 1), f32)
        inner = jnp.zeros((ROW_STEP, 1), f32)
        for j in range(groups):
            cols = pl.ds(j * bc, bc)
            x = tv[rows, cols].astype(f32)
            norm = own_text[j, core, y, rows].astype(f32) + mate_text[j, y, rows].astype(f32)
            for yy in far:
                norm = norm + far_text[yy, j, rows].astype(f32)
            scaled = gain_ref[:, cols] * norm
            squares += jnp.sum(x * x, axis=1, keepdims=True)
            inner += jnp.sum(x * scaled, axis=1, keepdims=True)
        inv = lax.rsqrt(squares / width + norm_eps)
        pull = inv**3 * (inner / width)
        for j in range(groups):
            cols = pl.ds(j * bc, bc)
            x = tv[rows, cols].astype(f32)
            norm = own_text[j, core, y, rows].astype(f32) + mate_text[j, y, rows].astype(f32)
            for yy in far:
                norm = norm + far_text[yy, j, rows].astype(f32)
            text_out[rows, cols] = (inv * (gain_ref[:, cols] * norm) - x * pull).astype(bf16)

    to_copy = pltpu.make_async_copy(text_out, text_hbm_out, to_sem)
    to_copy.start()

    def finish(chunk, j):
        proj_out[pl.ds(j, shard_k, stride=fold), :] = chunk.astype(f32).T

    finish(o_out[me], me)
    for t in reversed(range(last)):
        o_from(t).wait_recv()
        finish(o_in[targets[t]], targets[t])

    vision.drain()
    for t in range(last):
        w_to(t).wait_send()
        n_to(t).wait_send()
        o_to(t).wait_send()
    for k in range(len(beside)):
        stat_to(k).wait_send()
    for o in range(1, depth):
        line_to(o).wait_send()
    for k in range(len(order)):
        text_to_mate(k).wait_send()
        for yy in far:
            text_to_far(k, yy).wait_send()
    for yy in far + [y]:
        image_to_mate(yy).wait_send()
    for yy in far:
        for t in range(shards):
            image_to_far(yy, t).wait_send()
    to_copy.wait()


def place_outputs(text_in, proj_in, text_out, proj_out, text_held, proj_held, in_sem, out_sem):
    def copies(refs, sem):
        found = []
        for k, (src, dst) in enumerate(refs):
            step = src.shape[0] // PIECES
            for p in range(PIECES):
                rows = pl.ds(p * step, step)
                found.append(pltpu.make_async_copy(src.at[rows], dst.at[rows], sem.at[k, p]))
        return found

    into = copies(((text_in, text_held), (proj_in, proj_held)), in_sem)
    back = copies(((text_held, text_out), (proj_held, proj_out)), out_sem)
    for copy in into:
        copy.start()
    for first, second in zip(into, back):
        first.wait()
        second.start()
    for copy in back:
        copy.wait()


def live_rows(image_count, groups):
    image_rows = IMG_MAX * PATCH
    row_ids = jnp.arange(groups * image_rows, dtype=jnp.int32)
    owners = row_ids // image_rows
    slot_ids = row_ids % image_rows // PATCH
    owner_match = owners[:, None] == jnp.arange(groups, dtype=jnp.int32)[None, :]
    owner_counts = jnp.sum(jnp.where(owner_match, image_count[None, :], 0), axis=1)
    return (slot_ids < owner_counts)[:, None]


def fused_body(vision_rows, image_count, proj_flat, text_embeds, norm_gain, q_weight, q_grad):
    groups, shards = lax.axis_size("mp"), lax.axis_size("dp")
    model_width, bc = q_weight.shape
    image_rows, enc_width = vision_rows.shape
    text_rows = text_embeds.shape[0]
    shard_k = proj_flat.shape[0] * proj_flat.shape[1] // bc
    span = bc // shards
    chips, depth = groups // CORES, shards // SIDE
    all_rows = shards * image_rows
    grad_scale = 1.0 / float(all_rows) ** 0.5
    f32, bf16 = jnp.float32, jnp.bfloat16
    vmem, dma = pltpu.VMEM, pltpu.SemaphoreType.DMA
    on_chip = pl.BlockSpec(memory_space=pltpu.VMEM)
    scalars = pl.BlockSpec(memory_space=pltpu.SMEM)
    anywhere = pl.BlockSpec(memory_space=pl.ANY)
    text_grad, proj_block = pl.pallas_call(
        functools.partial(kernel, shards, groups, grad_scale),
        name="projector_backward",
        out_shape=(
            jax.ShapeDtypeStruct(text_embeds.shape, bf16),
            jax.ShapeDtypeStruct(proj_flat.shape, f32),
        ),
        in_specs=[scalars] + [anywhere] * 6,
        out_specs=(anywhere, on_chip),
        scratch_shapes=[
            vmem(proj_flat.shape, bf16),
            vmem((all_rows, enc_width), bf16),
            vmem((1, model_width), f32),
            vmem((image_rows, bc), bf16),
            vmem((groups * text_rows, bc), bf16),
            vmem((groups, bc, bc), bf16),
            vmem(text_embeds.shape, bf16),
            vmem(text_embeds.shape, bf16),
            vmem((groups, CORES, chips, text_rows, bc), bf16),
            vmem((groups, bc, image_rows), bf16),
            vmem((groups, chips, text_rows, bc), bf16),
            vmem((chips, bc, image_rows), bf16),
            vmem((groups, chips, text_rows, bc), bf16),
            vmem((chips, bc, image_rows), bf16),
            vmem((chips, groups, text_rows, bc), bf16),
            vmem((chips, bc, image_rows), bf16),
            vmem(proj_flat.shape, f32),
            vmem((shards, span, shard_k), bf16),
            vmem((span, enc_width), bf16),
            vmem((shards, span, image_rows), bf16),
            vmem((span, all_rows), bf16),
            vmem((span, all_rows), bf16),
            vmem((span, all_rows), bf16),
            vmem((span, image_rows), f32),
            vmem((shards, span, shard_k), bf16),
            vmem((shards, span, shard_k), bf16),
            vmem((2 * shards, image_rows), f32),
            vmem((SIDE * groups, 2 * shards, image_rows), f32),
            vmem((2 * shards, image_rows), f32),
            vmem((depth, 2 * shards, image_rows), f32),
            dma, dma, dma, dma((2, groups)), dma((groups,)), dma, dma,
            dma((3, depth, CHUNKS)), dma((shards, CHUNKS)), dma((shards, CHUNKS)), dma((shards, CHUNKS)),
            dma((shards,)), dma((shards,)), dma((shards,)), dma((shards,)), dma((shards,)), dma((shards,)),
            dma((groups,)), dma((groups,)),
            dma((chips,)), dma((chips,)),
            dma((groups, chips)), dma((chips, groups)),
            dma((chips, shards)), dma((chips, shards)),
            dma((SIDE * groups,)), dma((SIDE * groups,)),
            dma((depth,)), dma((depth,)),
        ],
        compiler_params=pltpu.CompilerParams(
            collective_id=0, has_side_effects=True, vmem_limit_bytes=56 * 1024 * 1024
        ),
    )(
        image_count,
        proj_flat,
        vision_rows,
        norm_gain[None, :],
        q_grad,
        q_weight.reshape(groups, bc, bc),
        text_embeds,
    )
    kinds = (text_grad, proj_block)
    return pl.pallas_call(
        place_outputs,
        name="place_outputs",
        out_shape=tuple(jax.ShapeDtypeStruct(a.shape, a.dtype) for a in kinds),
        in_specs=[anywhere] * 2,
        out_specs=(anywhere, anywhere),
        scratch_shapes=[vmem(a.shape, a.dtype) for a in kinds] + [dma((2, PIECES)), dma((2, PIECES))],
    )(*kinds)


def norm_back(rows_in, grads, gain):
    inputs = rows_in.astype(jnp.float32)
    inv_rms = lax.rsqrt(jnp.mean(inputs * inputs, axis=-1, keepdims=True) + norm_eps)
    scaled = gain[None, :] * grads
    inner_mean = jnp.mean(scaled * inputs, axis=-1, keepdims=True)
    return inv_rms * scaled - inputs * inv_rms**3 * inner_mean


def general_body(vision_rows, image_count, proj_flat, text_embeds, norm_gain, q_weight, q_grad):
    groups = lax.axis_size("mp")
    member = lax.axis_index("mp")
    shards = lax.axis_size("dp")
    enc_width = vision_rows.shape[1]
    block_cols = q_weight.shape[1]
    model_width = q_weight.shape[0]
    used_count = enc_width * block_cols
    image_rows = IMG_MAX * PATCH
    gathered = lax.all_gather(proj_flat, "dp", axis=0, tiled=True)
    proj_block = gathered.reshape(-1)[:used_count].reshape(enc_width, block_cols)
    embed_cols = jnp.dot(vision_rows, proj_block, preferred_element_type=jnp.float32).astype(
        jnp.bfloat16
    )
    live_group = live_rows(image_count, groups)
    blocks = q_grad.reshape(groups, ROWS_DEV, block_cols)
    image_query = blocks[:, :image_rows].reshape(-1, block_cols)
    text_query = blocks[:, image_rows:].reshape(-1, block_cols)
    image_term = row_term(image_query, q_weight)
    image_norm = lax.psum_scatter(
        image_term.astype(jnp.bfloat16), "mp", scatter_dimension=1, tiled=True
    ).astype(jnp.float32)
    text_norm = lax.psum_scatter(
        row_term(text_query, q_weight).astype(jnp.bfloat16), "mp", scatter_dimension=0, tiled=True
    ).astype(jnp.float32)
    x_cols = embed_cols.astype(jnp.float32)
    gain_cols = lax.dynamic_slice_in_dim(norm_gain, member * block_cols, block_cols)
    scaled = gain_cols[None, :] * image_norm
    squares, inner_sum = lax.psum(
        (jnp.sum(x_cols * x_cols, axis=1), jnp.sum(scaled * x_cols, axis=1)), "mp"
    )
    inv_rms = lax.rsqrt(squares / model_width + norm_eps)[:, None]
    image_input = inv_rms * scaled - x_cols * inv_rms**3 * (inner_sum / model_width)[:, None]
    image_cols = jnp.where(live_group, image_input, 0.0).astype(jnp.bfloat16)
    text_grad = norm_back(text_embeds, text_norm, norm_gain).astype(jnp.bfloat16)
    grad_scale = 1.0 / jnp.sqrt(jnp.float32(shards * groups * image_rows))
    proj_part = (
        lax.dot_general(
            vision_rows, image_cols, (((0,), (0,)), ((), ())), preferred_element_type=jnp.float32
        )
        * grad_scale
    )
    stored_rows = proj_flat.shape[0]
    padded = jnp.pad(proj_part.reshape(-1), (0, shards * stored_rows * 128 - used_count))
    padded = padded.reshape(shards * stored_rows, 128)
    proj_grad = lax.psum_scatter(padded, "dp", scatter_dimension=0, tiled=True)
    return (text_grad, proj_grad)


def body(vision_rows, image_count, proj_flat, text_embeds, norm_gain, q_weight, q_grad):
    groups, shards = lax.axis_size("mp"), lax.axis_size("dp")
    bc = q_weight.shape[1]
    count = proj_flat.shape[0] * proj_flat.shape[1]
    shard_k = count // bc
    fits = (
        count % bc == 0
        and shard_k == LANES
        and bc == shards * LANES
        and shard_k * shards == vision_rows.shape[1]
        and shard_k == vision_rows.shape[0]
        and bc % TILE == 0
        and groups > CORES
        and groups % CORES == 0
        and vision_rows.shape[0] // groups % ROW_STEP == 0
        and text_embeds.shape[0] % (PIECES * ROW_STEP) == 0
        and shards > SIDE
        and shards % SIDE == 0
    )
    run = fused_body if fits else general_body
    return run(vision_rows, image_count, proj_flat, text_embeds, norm_gain, q_weight, q_grad)


def solution(mesh):
    return jax.shard_map(
        body,
        mesh=mesh,
        in_specs=(
            P("dp", None),
            P("dp"),
            P(("dp", "mp"), None),
            P(("dp", "mp"), None),
            P(),
            P(None, "mp"),
            P("dp", "mp"),
        ),
        out_specs=(P(("dp", "mp"), None), P(("dp", "mp"), None)),
        check_vma=False,
    )
```

```python
import functools

import jax
import jax.numpy as jnp
from jax import lax
from jax.experimental import pallas as pl
from jax.experimental.pallas import tpu as pltpu
from jax.sharding import PartitionSpec as P

IMG_MAX = 4
PATCH = 8
ROWS_DEV = 128
CORES = 2
SIDE = 2
CHUNKS = 4
PIECES = 2
LANES = 128
ROW_STEP = 16

MESH = pl.DeviceIdType.MESH

norm_eps = 1e-05


def row_term(left, weight):
    return lax.dot_general(
        left, weight, (((1,), (1,)), ((), ())), preferred_element_type=jnp.float32
    )


def remote(src, dst, send, recv, device):
    return pltpu.make_async_remote_copy(
        src_ref=src, dst_ref=dst, send_sem=send, recv_sem=recv,
        device_id=device, device_id_type=MESH,
    )


class VisionGather:
    def __init__(self, depth, me, member, buf, block_rows, send, recv, mate_send, mate_recv):
        self.depth, self.me, self.member = depth, me, member
        self.z, self.x = me // SIDE, me % SIDE
        self.core = member % CORES
        self.mate = member + 1 - 2 * self.core
        self.buf, self.block_rows = buf, block_rows
        self.send, self.recv = send, recv
        self.mate_send, self.mate_recv = mate_send, mate_recv
        self.half = block_rows // CORES
        self.step = self.half // CHUNKS

    def place(self, block, chunk, core):
        first = block * self.block_rows + core * self.half + chunk * self.step
        return self.buf.at[pl.ds(pl.multiple_of(first, self.step), self.step)]

    def copy(self, zz, x, chunk, way):
        block = zz * SIDE + x
        place = self.place(block, chunk, self.core)
        target = (self.me + SIDE, self.me - SIDE, self.z * SIDE + 1 - self.x)[way]
        return remote(
            place, place, self.send.at[way], self.recv.at[block, chunk],
            (target, self.member),
        )

    def to_mate(self, block, chunk):
        place = self.place(block, chunk, self.core)
        return remote(
            place, place, self.mate_send, self.mate_recv.at[block],
            (self.me, self.mate),
        )

    def from_mate(self, block):
        first = block * self.block_rows + (1 - self.core) * self.half
        place = self.buf.at[pl.ds(pl.multiple_of(first, self.half), self.half)]
        return remote(place, place, self.mate_send, self.mate_recv.at[block], (self.me, self.mate))

    def sent(self, send, blocks):
        place = self.buf.at[pl.ds(0, blocks * self.half)]
        remote(place, place, send, self.mate_recv.at[0], (self.me, self.mate)).wait_send()

    def start(self):
        for chunk in range(CHUNKS):
            @pl.when(self.z < self.depth - 1)
            def _():
                self.copy(self.z, self.x, chunk, 0).start()

            @pl.when(self.z > 0)
            def _():
                self.copy(self.z, self.x, chunk, 1).start()

            self.copy(self.z, self.x, chunk, 2).start()

    def relay(self, hop, chunk):
        below, above = self.z - hop, self.z + hop

        @pl.when(below >= 0)
        def _():
            self.copy(below, self.x, chunk, 0).wait_recv()

            @pl.when(self.z < self.depth - 1)
            def _():
                self.copy(below, self.x, chunk, 0).start()

            self.copy(below, self.x, chunk, 2).start()
            self.to_mate(below * SIDE + self.x, chunk).start()

        @pl.when(above < self.depth)
        def _():
            self.copy(above, self.x, chunk, 1).wait_recv()

            @pl.when(self.z > 0)
            def _():
                self.copy(above, self.x, chunk, 1).start()

            self.copy(above, self.x, chunk, 2).start()
            self.to_mate(above * SIDE + self.x, chunk).start()

    def levels(self, hop, use):
        for zz in (self.z,) if hop == 0 else (self.z - hop, self.z + hop):
            @pl.when((zz >= 0) & (zz < self.depth))
            def _():
                use(zz)

    def side(self, hop, chunk):
        def take(zz):
            self.copy(zz, 1 - self.x, chunk, 2).wait_recv()
            self.to_mate(zz * SIDE + 1 - self.x, chunk).start()

        self.levels(hop, take)

    def arrive(self, zz):
        @pl.when(zz != self.z)
        def _():
            self.from_mate(zz * SIDE + self.x).wait_recv()

        self.from_mate(zz * SIDE + 1 - self.x).wait_recv()

    def drain(self):
        for zz in range(self.depth):
            @pl.when(self.z == zz)
            def _():
                if zz < self.depth - 1:
                    self.sent(self.send.at[0], zz + 1)
                if zz > 0:
                    self.sent(self.send.at[1], self.depth - zz)
        self.sent(self.send.at[2], self.depth)
        self.sent(self.mate_send, SIDE * self.depth - 1)


def kernel(
    shards, groups, grad_scale,
    count_ref, proj_hbm, vision_hbm, gain_hbm, q_hbm, w_hbm, text_hbm,
    text_out, proj_out,
    pv, vv, gain_ref, q_image, q_text, wv, tv,
    own_text, own_image, mate_text, mate_image, sum_text, sum_image,
    far_text, far_image, w_flat, w_out, wt, n_out, nt, xt, gt, gain_t, o_out, o_in,
    stat_f32, stat_own, stat_near, stat_sum, stat_far,
    p_sem, vis_sem, gain_sem, q_sem, w_sem, t_sem,
    v_send, v_recv, vm_send, vm_recv, wt_send, wt_recv, n_send, n_recv, o_send, o_recv,
    mt_send, mt_recv, mi_send, mi_recv, ft_send, ft_recv, fi_send, fi_recv,
    s_send, s_recv, z_send, z_recv, up_sem, down_sem,
):
    me, member = lax.axis_index("dp"), lax.axis_index("mp")
    depth = shards // SIDE
    chips = groups // CORES
    y, core = member // CORES, member % CORES
    mate = y * CORES + 1 - core
    z, x = me // SIDE, me % SIDE
    bc = wv.shape[1]
    span = bc // shards
    fold = bc // LANES
    shard_k = wt.shape[1] // shards
    image_rows = q_image.shape[0]
    per_image = image_rows // groups
    text_rows = tv.shape[0]
    rows_dev = per_image + text_rows
    width = groups * bc
    f32, bf16 = jnp.float32, jnp.bfloat16

    far = [lax.rem(y + step, chips) for step in range(1, chips)]
    order = [yy * CORES + lax.rem(core + flip, CORES) for yy in far + [y] for flip in (1, 0)]
    early = len(order) - CORES
    offsets = sorted(range(1, depth), key=lambda o: -min(o, depth - o)) + [0]
    targets = [
        lax.rem(z + o, depth) * SIDE + (x if flip else 1 - x) for o in offsets for flip in (0, 1)
    ]
    last = shards - 1

    p_copy = pltpu.make_async_copy(proj_hbm, pv, p_sem)
    p_copy.start()
    own_rows = pl.ds(pl.multiple_of(me * image_rows, image_rows), image_rows)
    vis_copy = pltpu.make_async_copy(vision_hbm, vv.at[own_rows], vis_sem)
    vis_copy.start()
    q_copies = [
        pltpu.make_async_copy(
            q_hbm.at[pl.ds(g * rows_dev + first, count)], dst.at[pl.ds(g * count, count)], q_sem.at[k]
        )
        for k, (first, count, dst) in enumerate(((0, per_image, q_image), (per_image, text_rows, q_text)))
        for g in range(groups)
    ]
    q_image_done = pltpu.make_async_copy(q_hbm.at[pl.ds(0, image_rows)], q_image, q_sem.at[0])
    q_text_done = pltpu.make_async_copy(q_hbm.at[pl.ds(0, groups * text_rows)], q_text, q_sem.at[1])
    w_copies = [pltpu.make_async_copy(w_hbm.at[j], wv.at[j], w_sem.at[k]) for k, j in enumerate(order)]
    gain_copy = pltpu.make_async_copy(gain_hbm, gain_ref, gain_sem)
    t_copy = pltpu.make_async_copy(text_hbm, tv, t_sem)
    for copy in q_copies[:groups] + w_copies[:1]:
        copy.start()

    barrier = pltpu.get_barrier_semaphore()
    across = z * SIDE + 1 - x
    beside = [(me, lax.rem(member + step, groups)) for step in range(1, groups)]
    beside += [(across, lax.rem(member + step, groups)) for step in range(groups)]
    for device in beside:
        pl.semaphore_signal(barrier, inc=1, device_id=device, device_id_type=MESH)

    @pl.when(z > 0)
    def _():
        pl.semaphore_signal(barrier, inc=1, device_id=(me - SIDE, member), device_id_type=MESH)

    @pl.when(z < depth - 1)
    def _():
        pl.semaphore_signal(barrier, inc=1, device_id=(me + SIDE, member), device_id_type=MESH)

    def pass_on(hop):
        @pl.when(z == hop)
        def _():
            if hop > 0:
                pl.semaphore_wait(up_sem, 1)
            if hop < depth - 1:
                pl.semaphore_signal(up_sem, inc=1, device_id=(me + SIDE, member), device_id_type=MESH)

        @pl.when(depth - 1 - z == hop)
        def _():
            if hop > 0:
                pl.semaphore_wait(down_sem, 1)
            if hop < depth - 1:
                pl.semaphore_signal(down_sem, inc=1, device_id=(me - SIDE, member), device_id_type=MESH)

    vis_copy.wait()
    for copy in w_copies[1:] + q_copies[groups:] + [gain_copy, t_copy]:
        copy.start()

    @pl.when((z == 0) | (z == depth - 1))
    def _():
        pl.semaphore_wait(barrier, len(beside) + 1)

    @pl.when((z > 0) & (z < depth - 1))
    def _():
        pl.semaphore_wait(barrier, len(beside) + 2)

    vision = VisionGather(depth, me, member, vv, image_rows, v_send, v_recv, vm_send, vm_recv)
    vision.start()
    pass_on(0)

    p_copy.wait()
    w_flat[...] = pv[...].astype(f32)
    for j in range(shards):
        w_out[j] = w_flat[pl.ds(j, shard_k, stride=fold), :].astype(bf16).T
    own_k = pl.ds(pl.multiple_of(me * shard_k, shard_k), shard_k)
    wt[:, own_k] = w_out[me]

    def w_to(t):
        j = targets[t]
        return remote(w_out.at[j], wt.at[:, own_k], wt_send, wt_recv, (j, member))

    def all_to(buf, send, recv):
        place = buf.at[pl.ds(0, last)]
        return remote(place, place, send, recv, (me, mate))

    def text_to_mate(k):
        j = order[k]
        return remote(own_text.at[j, 1 - core], mate_text.at[j], mt_send, mt_recv.at[j], (me, mate))

    def image_to_mate(yy):
        return remote(
            own_image.at[yy * CORES + 1 - core], mate_image.at[yy],
            mi_send, mi_recv.at[yy], (me, mate),
        )

    def text_to_far(k, yy):
        j = order[k]
        return remote(
            sum_text.at[j, yy], far_text.at[y, j], ft_send, ft_recv, (me, yy * CORES + core)
        )

    def piece(t):
        return pl.ds(pl.multiple_of(targets[t] * span, span), span)

    def image_to_far(yy, t):
        return remote(
            sum_image.at[yy, piece(t)], far_image.at[y, piece(t)],
            fi_send, fi_recv.at[y, t], (me, yy * CORES + core),
        )

    def image_from_far(yy, t):
        return remote(
            sum_image.at[yy, piece(t)], far_image.at[yy, piece(t)],
            fi_send, fi_recv.at[yy, t], (me, yy * CORES + core),
        )

    def image_multiply(k):
        j = order[k]
        w_copies[k].wait()

        @pl.loop(0, 1)
        def _(n):
            rows = pl.ds(pl.multiple_of(n * bc, bc), bc)
            own_image[j, rows] = row_term(wv[j, rows], q_image[...]).astype(bf16)

        if k % CORES == 0:
            image_to_mate((far + [y])[k // CORES]).start()

    def text_multiply(k):
        j = order[k]
        term = row_term(q_text[...], wv[j]).astype(bf16)
        for g in range(groups):
            own_text[j, g % CORES, g // CORES] = term[g * text_rows : (g + 1) * text_rows]
        text_to_mate(k).start()

    def add_image(yy):
        image_to_mate(yy).wait_recv()
        for t in range(shards):
            rows = piece(t)
            total = own_image[yy * CORES + core, rows].astype(f32) + mate_image[yy, rows].astype(f32)
            sum_image[yy, rows] = total.astype(bf16)
            image_to_far(yy, t).start()

    def add_text(k):
        j = order[k]
        text_to_mate(k).wait_recv()
        for yy in far:
            @pl.loop(0, text_rows // ROW_STEP)
            def _(n):
                rows = pl.ds(pl.multiple_of(n * ROW_STEP, ROW_STEP), ROW_STEP)
                total = own_text[j, core, yy, rows].astype(f32) + mate_text[j, yy, rows].astype(f32)
                sum_text[j, yy, rows] = total.astype(bf16)
            text_to_far(k, yy).start()

    lanes = lax.broadcasted_iota(jnp.int32, (span, image_rows), 1)
    slots = lax.rem(lanes, per_image)
    held = jnp.zeros((span, image_rows), jnp.int32)
    for g in range(groups):
        held = jnp.where(lanes // per_image == g, count_ref[g] * PATCH, held)
    live = slots < held

    def n_to(t):
        j = targets[t]
        return remote(n_out.at[t], nt.at[:, own_lanes], n_send, n_recv, (j, member))

    own_lanes = pl.ds(pl.multiple_of(me * image_rows, image_rows), image_rows)

    def spread_image(t):
        if t == 0:
            image_to_mate(y).wait_recv()
        for yy in far:
            image_from_far(yy, t).wait_recv()
        rows = piece(t)
        total = own_image[member, rows].astype(f32) + mate_image[y, rows].astype(f32)
        for yy in far:
            total = total + far_image[yy, rows].astype(f32)
        total = jnp.where(live, total, 0.0).astype(bf16)
        if t < last:
            n_out[t] = total
            n_to(t).start()
        else:
            nt[:, own_lanes] = total

    def each(action, *lead):
        return [functools.partial(action, *lead, chunk) for chunk in range(CHUNKS)]

    def play(*actions):
        for action in actions:
            action()

    images = [functools.partial(spread_image, t) for t in range(shards)]

    first, rest = each(vision.relay, 1)[:2], each(vision.relay, 1)[2:]
    q_image_done.wait()
    for k in range(len(order)):
        image_multiply(k)
        if k + 1 < depth - 1:
            pass_on(k + 1)
        if k % CORES == 0 and k >= CORES:
            add_image(far[k // CORES - 1])
            if k == CORES:
                play(*first)
    for hop in range(min(len(order) + 1, depth - 1), depth):
        pass_on(hop)
    play(*rest)
    for t in range(last):
        w_to(t).start()
    q_text_done.wait()
    text_multiply(0)
    play(*each(vision.side, 0))
    play(*images[:1])
    text_multiply(1)
    play(*images[1:2])
    add_text(0)
    waves = [each(vision.relay, hop) for hop in range(2, depth)]
    flow = [action for wave in waves for action in wave]
    for k in range(2, len(order)):
        text_multiply(k)
        play(*images[2 * k - 2 : 2 * k])
        play(*flow[2 * k - 4 : 2 * k - 2])
        if k == 2:
            add_text(1)
    play(*images[2 * len(order) - 2 :])
    gain_copy.wait()
    own_gain = gain_ref[:, pl.ds(pl.multiple_of(member * bc + me * span, span), span)]
    gain_t[...] = jnp.broadcast_to(own_gain, (image_rows, span)).T
    play(*each(vision.side, 1))
    play(*flow[2 * len(order) - 4 :])
    all_to(w_out, wt_send, wt_recv).wait_recv()

    def embed(zz):
        vision.arrive(zz)
        pair = pl.ds(pl.multiple_of(zz * SIDE * image_rows, SIDE * image_rows), SIDE * image_rows)
        rounded = row_term(wt[...], vv[pair]).astype(bf16)
        xt[:, pair] = rounded
        value = rounded.astype(f32)
        squares = jnp.sum(value * value, axis=0, keepdims=True)
        for s in range(SIDE):
            stat_f32[pl.ds(zz * SIDE + s, 1)] = squares[:, s * image_rows : (s + 1) * image_rows]

    for hop in range(depth):
        if hop >= 2:
            play(*each(vision.side, hop))
        if hop < depth - 1:
            vision.levels(hop, embed)
    vision.levels(depth - 1, embed)

    all_to(n_out, n_send, n_recv).wait_recv()
    for j in range(shards):
        cols = pl.ds(j * image_rows, image_rows)
        scaled = gain_t[...] * nt[:, cols].astype(f32)
        inner = jnp.sum(scaled * xt[:, cols].astype(f32), axis=0, keepdims=True)
        stat_f32[pl.ds(shards + j, 1)] = inner
    stat_own[...] = stat_f32[...].astype(bf16)

    def stat_to(k):
        device = beside[k]
        mine = lax.rem(me, SIDE) * groups + member
        return remote(stat_own, stat_near.at[mine], s_send, s_recv, device)

    near_done = pl.ds(0, len(beside))
    stat_near_done = remote(
        stat_near.at[near_done], stat_near.at[near_done], s_send, s_recv, (me, mate)
    )
    for k in range(len(beside)):
        stat_to(k).start()
    for k in range(2, len(order)):
        add_text(k)
    total = stat_f32[...]
    stat_near_done.wait_recv()
    for device in beside:
        total = total + stat_near[lax.rem(device[0], SIDE) * groups + device[1]].astype(f32)
    stat_sum[...] = total.astype(bf16)

    def line_to(o):
        target = lax.rem(z + o, depth)
        return remote(stat_sum, stat_far.at[z], z_send, z_recv, (target * SIDE + x, member))

    far_done = pl.ds(0, depth - 1)
    stat_far_done = remote(
        stat_far.at[far_done], stat_far.at[far_done], z_send, z_recv, (me, mate)
    )
    for o in range(1, depth):
        line_to(o).start()
    stat_far_done.wait_recv()
    for o in range(1, depth):
        total = total + stat_far[lax.rem(z + o, depth)].astype(f32)

    inv_all = lax.rsqrt(total[:shards] / width + norm_eps)
    pull_all = inv_all**3 * (total[shards:] / width)
    for b in range(shards):
        cols = pl.ds(b * image_rows, image_rows)
        scaled = gain_t[...] * nt[:, cols].astype(f32)
        grad = inv_all[b : b + 1] * scaled - xt[:, cols].astype(f32) * pull_all[b : b + 1]
        gt[:, cols] = grad.astype(bf16)

    def o_to(t):
        j = targets[t]
        return remote(o_out.at[j], o_in.at[me], o_send, o_recv.at[me], (j, member))

    def o_from(t):
        j = targets[t]
        return remote(o_out.at[j], o_in.at[j], o_send, o_recv.at[j], (j, member))

    out = (jnp.dot(gt[...], vv[...], preferred_element_type=f32) * grad_scale).astype(bf16)
    for j in range(shards):
        o_out[j] = out[:, j * shard_k : (j + 1) * shard_k]
    for t in range(last):
        o_to(t).start()

    text_far = sum_text.at[:, pl.ds(0, len(far))]
    text_far_done = remote(text_far, text_far, ft_send, ft_recv, (me, mate))
    text_far_done.wait_recv()
    t_copy.wait()

    @pl.loop(0, text_rows // ROW_STEP)
    def _(n):
        rows = pl.ds(pl.multiple_of(n * ROW_STEP, ROW_STEP), ROW_STEP)
        squares = jnp.zeros((ROW_STEP, 1), f32)
        inner = jnp.zeros((ROW_STEP, 1), f32)
        for j in range(groups):
            cols = pl.ds(j * bc, bc)
            x = tv[rows, cols].astype(f32)
            norm = own_text[j, core, y, rows].astype(f32) + mate_text[j, y, rows].astype(f32)
            for yy in far:
                norm = norm + far_text[yy, j, rows].astype(f32)
            scaled = gain_ref[:, cols] * norm
            squares += jnp.sum(x * x, axis=1, keepdims=True)
            inner += jnp.sum(x * scaled, axis=1, keepdims=True)
        inv = lax.rsqrt(squares / width + norm_eps)
        pull = inv**3 * (inner / width)
        for j in range(groups):
            cols = pl.ds(j * bc, bc)
            x = tv[rows, cols].astype(f32)
            norm = own_text[j, core, y, rows].astype(f32) + mate_text[j, y, rows].astype(f32)
            for yy in far:
                norm = norm + far_text[yy, j, rows].astype(f32)
            text_out[rows, cols] = (inv * (gain_ref[:, cols] * norm) - x * pull).astype(bf16)

    def finish(chunk, j):
        proj_out[pl.ds(j, shard_k, stride=fold), :] = chunk.astype(f32).T

    finish(o_out[me], me)
    for t in reversed(range(last)):
        o_from(t).wait_recv()
        finish(o_in[targets[t]], targets[t])

    vision.drain()
    all_to(w_out, wt_send, wt_recv).wait_send()
    all_to(n_out, n_send, n_recv).wait_send()
    all_to(o_out, o_send, o_recv.at[0]).wait_send()
    stat_near_done.wait_send()
    stat_far_done.wait_send()
    text_far_done.wait_send()
    remote(mate_text, mate_text, mt_send, mt_recv.at[0], (me, mate)).wait_send()
    remote(mate_image, mate_image, mi_send, mi_recv.at[0], (me, mate)).wait_send()
    image_far = sum_image.at[pl.ds(0, len(far))]
    remote(image_far, image_far, fi_send, fi_recv.at[0, 0], (me, mate)).wait_send()


def place_outputs(text_in, proj_in, text_out, proj_out, sem):
    copies = []
    for k, (src, dst) in enumerate(((text_in, text_out), (proj_in, proj_out))):
        step = src.shape[0] // PIECES
        for p in range(PIECES):
            rows = pl.ds(p * step, step)
            copies.append(pltpu.make_async_copy(src.at[rows], dst.at[rows], sem.at[k, p]))
    for copy in copies:
        copy.start()
    for copy in copies:
        copy.wait()


def live_rows(image_count, groups):
    image_rows = IMG_MAX * PATCH
    row_ids = jnp.arange(groups * image_rows, dtype=jnp.int32)
    owners = row_ids // image_rows
    slot_ids = row_ids % image_rows // PATCH
    owner_match = owners[:, None] == jnp.arange(groups, dtype=jnp.int32)[None, :]
    owner_counts = jnp.sum(jnp.where(owner_match, image_count[None, :], 0), axis=1)
    return (slot_ids < owner_counts)[:, None]


def fused_body(vision_rows, image_count, proj_flat, text_embeds, norm_gain, q_weight, q_grad):
    groups, shards = lax.axis_size("mp"), lax.axis_size("dp")
    model_width, bc = q_weight.shape
    image_rows, enc_width = vision_rows.shape
    text_rows = text_embeds.shape[0]
    shard_k = proj_flat.shape[0] * proj_flat.shape[1] // bc
    span = bc // shards
    chips, depth = groups // CORES, shards // SIDE
    all_rows = shards * image_rows
    grad_scale = 1.0 / float(all_rows) ** 0.5
    f32, bf16 = jnp.float32, jnp.bfloat16
    vmem, dma = pltpu.VMEM, pltpu.SemaphoreType.DMA
    on_chip = pl.BlockSpec(memory_space=pltpu.VMEM)
    scalars = pl.BlockSpec(memory_space=pltpu.SMEM)
    in_hbm = pl.BlockSpec(memory_space=pltpu.HBM)
    text_grad, proj_block = pl.pallas_call(
        functools.partial(kernel, shards, groups, grad_scale),
        name="projector_backward",
        out_shape=(vmem(text_embeds.shape, bf16), vmem(proj_flat.shape, f32)),
        in_specs=[scalars] + [in_hbm] * 6,
        out_specs=(on_chip, on_chip),
        scratch_shapes=[
            vmem(proj_flat.shape, bf16),
            vmem((all_rows, enc_width), bf16),
            vmem((1, model_width), f32),
            vmem((image_rows, bc), bf16),
            vmem((groups * text_rows, bc), bf16),
            vmem((groups, bc, bc), bf16),
            vmem(text_embeds.shape, bf16),
            vmem((groups, CORES, chips, text_rows, bc), bf16),
            vmem((groups, bc, image_rows), bf16),
            vmem((groups, chips, text_rows, bc), bf16),
            vmem((chips, bc, image_rows), bf16),
            vmem((groups, chips, text_rows, bc), bf16),
            vmem((chips, bc, image_rows), bf16),
            vmem((chips, groups, text_rows, bc), bf16),
            vmem((chips, bc, image_rows), bf16),
            vmem(proj_flat.shape, f32),
            vmem((shards, span, shard_k), bf16),
            vmem((span, enc_width), bf16),
            vmem((shards, span, image_rows), bf16),
            vmem((span, all_rows), bf16),
            vmem((span, all_rows), bf16),
            vmem((span, all_rows), bf16),
            vmem((span, image_rows), f32),
            vmem((shards, span, shard_k), bf16),
            vmem((shards, span, shard_k), bf16),
            vmem((2 * shards, image_rows), f32),
            vmem((2 * shards, image_rows), bf16),
            vmem((SIDE * groups, 2 * shards, image_rows), bf16),
            vmem((2 * shards, image_rows), bf16),
            vmem((depth, 2 * shards, image_rows), bf16),
            dma, dma, dma, dma((2,)), dma((groups,)), dma,
            dma((3,)), dma((shards, CHUNKS)), dma, dma((shards,)),
            dma, dma, dma, dma, dma, dma((shards,)),
            dma, dma((groups,)), dma, dma((chips,)), dma, dma, dma, dma((chips, shards)),
            dma, dma, dma, dma, pltpu.SemaphoreType.REGULAR, pltpu.SemaphoreType.REGULAR,
        ],
        compiler_params=pltpu.CompilerParams(
            collective_id=0, has_side_effects=True, vmem_limit_bytes=56 * 1024 * 1024
        ),
    )(
        image_count,
        proj_flat,
        vision_rows,
        norm_gain[None, :],
        q_grad,
        q_weight.reshape(groups, bc, bc),
        text_embeds,
    )
    kinds = (text_grad, proj_block)
    return pl.pallas_call(
        place_outputs,
        name="place_outputs",
        out_shape=tuple(jax.ShapeDtypeStruct(a.shape, a.dtype) for a in kinds),
        in_specs=[on_chip] * 2,
        out_specs=(in_hbm, in_hbm),
        scratch_shapes=[dma((2, PIECES))],
        compiler_params=pltpu.CompilerParams(vmem_limit_bytes=4 * 1024 * 1024),
    )(*kinds)


def norm_back(rows_in, grads, gain):
    inputs = rows_in.astype(jnp.float32)
    inv_rms = lax.rsqrt(jnp.mean(inputs * inputs, axis=-1, keepdims=True) + norm_eps)
    scaled = gain[None, :] * grads
    inner_mean = jnp.mean(scaled * inputs, axis=-1, keepdims=True)
    return inv_rms * scaled - inputs * inv_rms**3 * inner_mean


def general_body(vision_rows, image_count, proj_flat, text_embeds, norm_gain, q_weight, q_grad):
    groups = lax.axis_size("mp")
    member = lax.axis_index("mp")
    shards = lax.axis_size("dp")
    enc_width = vision_rows.shape[1]
    block_cols = q_weight.shape[1]
    model_width = q_weight.shape[0]
    used_count = enc_width * block_cols
    image_rows = IMG_MAX * PATCH
    gathered = lax.all_gather(proj_flat, "dp", axis=0, tiled=True)
    proj_block = gathered.reshape(-1)[:used_count].reshape(enc_width, block_cols)
    embed_cols = jnp.dot(vision_rows, proj_block, preferred_element_type=jnp.float32).astype(
        jnp.bfloat16
    )
    live_group = live_rows(image_count, groups)
    blocks = q_grad.reshape(groups, ROWS_DEV, block_cols)
    image_query = blocks[:, :image_rows].reshape(-1, block_cols)
    text_query = blocks[:, image_rows:].reshape(-1, block_cols)
    image_term = row_term(image_query, q_weight)
    image_norm = lax.psum_scatter(
        image_term.astype(jnp.bfloat16), "mp", scatter_dimension=1, tiled=True
    ).astype(jnp.float32)
    text_norm = lax.psum_scatter(
        row_term(text_query, q_weight).astype(jnp.bfloat16), "mp", scatter_dimension=0, tiled=True
    ).astype(jnp.float32)
    x_cols = embed_cols.astype(jnp.float32)
    gain_cols = lax.dynamic_slice_in_dim(norm_gain, member * block_cols, block_cols)
    scaled = gain_cols[None, :] * image_norm
    squares, inner_sum = lax.psum(
        (jnp.sum(x_cols * x_cols, axis=1), jnp.sum(scaled * x_cols, axis=1)), "mp"
    )
    inv_rms = lax.rsqrt(squares / model_width + norm_eps)[:, None]
    image_input = inv_rms * scaled - x_cols * inv_rms**3 * (inner_sum / model_width)[:, None]
    image_cols = jnp.where(live_group, image_input, 0.0).astype(jnp.bfloat16)
    text_grad = norm_back(text_embeds, text_norm, norm_gain).astype(jnp.bfloat16)
    grad_scale = 1.0 / jnp.sqrt(jnp.float32(shards * groups * image_rows))
    proj_part = (
        lax.dot_general(
            vision_rows, image_cols, (((0,), (0,)), ((), ())), preferred_element_type=jnp.float32
        )
        * grad_scale
    )
    stored_rows = proj_flat.shape[0]
    padded = jnp.pad(proj_part.reshape(-1), (0, shards * stored_rows * 128 - used_count))
    padded = padded.reshape(shards * stored_rows, 128)
    proj_grad = lax.psum_scatter(padded, "dp", scatter_dimension=0, tiled=True)
    return (text_grad, proj_grad)


def body(vision_rows, image_count, proj_flat, text_embeds, norm_gain, q_weight, q_grad):
    groups, shards = lax.axis_size("mp"), lax.axis_size("dp")
    bc = q_weight.shape[1]
    count = proj_flat.shape[0] * proj_flat.shape[1]
    shard_k = count // bc
    fits = (
        count % bc == 0
        and shard_k == LANES
        and bc == shards * LANES
        and shard_k * shards == vision_rows.shape[1]
        and shard_k == vision_rows.shape[0]
        and groups > CORES
        and groups % CORES == 0
        and vision_rows.shape[0] // groups % ROW_STEP == 0
        and text_embeds.shape[0] % (PIECES * ROW_STEP) == 0
        and shards > SIDE
        and shards % SIDE == 0
    )
    run = fused_body if fits else general_body
    return run(vision_rows, image_count, proj_flat, text_embeds, norm_gain, q_weight, q_grad)


def solution(mesh):
    return jax.shard_map(
        body,
        mesh=mesh,
        in_specs=(
            P("dp", None),
            P("dp"),
            P(("dp", "mp"), None),
            P(("dp", "mp"), None),
            P(),
            P(None, "mp"),
            P("dp", "mp"),
        ),
        out_specs=(P(("dp", "mp"), None), P(("dp", "mp"), None)),
        check_vma=False,
    )
```

```python
import functools

import jax
import jax.numpy as jnp
from jax import lax
from jax.experimental import pallas as pl
from jax.experimental.pallas import tpu as pltpu
from jax.sharding import PartitionSpec as P

IMG_MAX = 4
PATCH = 8
ROWS_DEV = 128
CORES = 2
SIDE = 2
CHUNKS = 4
PIECES = 2
LANES = 128
TILE = 512
ROW_STEP = 16

MESH = pl.DeviceIdType.MESH

norm_eps = 1e-05


def row_term(left, weight):
    return lax.dot_general(
        left, weight, (((1,), (1,)), ((), ())), preferred_element_type=jnp.float32
    )


def remote(src, dst, send, recv, device):
    return pltpu.make_async_remote_copy(
        src_ref=src, dst_ref=dst, send_sem=send, recv_sem=recv,
        device_id=device, device_id_type=MESH,
    )


class VisionGather:
    def __init__(self, depth, me, member, buf, block_rows, send, recv, mate_send, mate_recv):
        self.depth, self.me, self.member = depth, me, member
        self.z, self.x = me // SIDE, me % SIDE
        self.core = member % CORES
        self.mate = member + 1 - 2 * self.core
        self.buf, self.block_rows = buf, block_rows
        self.send, self.recv = send, recv
        self.mate_send, self.mate_recv = mate_send, mate_recv
        self.half = block_rows // CORES
        self.step = self.half // CHUNKS

    def place(self, block, chunk, core):
        first = block * self.block_rows + core * self.half + chunk * self.step
        return self.buf.at[pl.ds(pl.multiple_of(first, self.step), self.step)]

    def copy(self, zz, x, chunk, way):
        block = zz * SIDE + x
        place = self.place(block, chunk, self.core)
        target = (self.me + SIDE, self.me - SIDE, self.z * SIDE + 1 - self.x)[way]
        return remote(
            place, place, self.send.at[way], self.recv.at[block, chunk],
            (target, self.member),
        )

    def to_mate(self, block, chunk):
        place = self.place(block, chunk, self.core)
        return remote(
            place, place, self.mate_send, self.mate_recv.at[block],
            (self.me, self.mate),
        )

    def from_mate(self, block):
        first = block * self.block_rows + (1 - self.core) * self.half
        place = self.buf.at[pl.ds(pl.multiple_of(first, self.half), self.half)]
        return remote(place, place, self.mate_send, self.mate_recv.at[block], (self.me, self.mate))

    def sent(self, send, blocks):
        place = self.buf.at[pl.ds(0, blocks * self.half)]
        remote(place, place, send, self.mate_recv.at[0], (self.me, self.mate)).wait_send()

    def start(self):
        for chunk in range(CHUNKS):
            @pl.when(self.z < self.depth - 1)
            def _():
                self.copy(self.z, self.x, chunk, 0).start()

            @pl.when(self.z > 0)
            def _():
                self.copy(self.z, self.x, chunk, 1).start()

            self.copy(self.z, self.x, chunk, 2).start()

    def relay(self, hop, chunk):
        below, above = self.z - hop, self.z + hop

        @pl.when(below >= 0)
        def _():
            self.copy(below, self.x, chunk, 0).wait_recv()

            @pl.when(self.z < self.depth - 1)
            def _():
                self.copy(below, self.x, chunk, 0).start()

            self.copy(below, self.x, chunk, 2).start()
            self.to_mate(below * SIDE + self.x, chunk).start()

        @pl.when(above < self.depth)
        def _():
            self.copy(above, self.x, chunk, 1).wait_recv()

            @pl.when(self.z > 0)
            def _():
                self.copy(above, self.x, chunk, 1).start()

            self.copy(above, self.x, chunk, 2).start()
            self.to_mate(above * SIDE + self.x, chunk).start()

    def levels(self, hop, use):
        for zz in (self.z,) if hop == 0 else (self.z - hop, self.z + hop):
            @pl.when((zz >= 0) & (zz < self.depth))
            def _():
                use(zz)

    def side(self, hop, chunk):
        def take(zz):
            self.copy(zz, 1 - self.x, chunk, 2).wait_recv()
            self.to_mate(zz * SIDE + 1 - self.x, chunk).start()

        self.levels(hop, take)

    def arrive(self, zz):
        @pl.when(zz != self.z)
        def _():
            self.from_mate(zz * SIDE + self.x).wait_recv()

        self.from_mate(zz * SIDE + 1 - self.x).wait_recv()

    def drain(self):
        for zz in range(self.depth):
            @pl.when(self.z == zz)
            def _():
                if zz < self.depth - 1:
                    self.sent(self.send.at[0], zz + 1)
                if zz > 0:
                    self.sent(self.send.at[1], self.depth - zz)
        self.sent(self.send.at[2], self.depth)
        self.sent(self.mate_send, SIDE * self.depth - 1)


def kernel(
    shards, groups, grad_scale,
    count_ref, proj_hbm, vision_hbm, gain_hbm, q_hbm, w_hbm, text_hbm,
    text_out, proj_out,
    pv, vv, gain_ref, q_image, q_text, wv, tv,
    own_text, own_image, mate_text, mate_image, sum_text, sum_image,
    far_text, far_image, w_flat, w_out, wt, n_out, nt, xt, gt, gain_t, o_out, o_in,
    stat_f32, stat_own, stat_near, stat_sum, stat_far,
    p_sem, vis_sem, gain_sem, q_sem, w_sem, t_sem,
    v_send, v_recv, vm_send, vm_recv, wt_send, wt_recv, n_send, n_recv, o_send, o_recv,
    mt_send, mt_recv, mi_send, mi_recv, ft_send, ft_recv, fi_send, fi_recv,
    s_send, s_recv, z_send, z_recv, up_sem, down_sem,
):
    me, member = lax.axis_index("dp"), lax.axis_index("mp")
    depth = shards // SIDE
    chips = groups // CORES
    y, core = member // CORES, member % CORES
    mate = y * CORES + 1 - core
    z, x = me // SIDE, me % SIDE
    bc = wv.shape[1]
    span = bc // shards
    fold = bc // LANES
    shard_k = wt.shape[1] // shards
    image_rows = q_image.shape[0]
    per_image = image_rows // groups
    text_rows = tv.shape[0]
    rows_dev = per_image + text_rows
    width = groups * bc
    f32, bf16 = jnp.float32, jnp.bfloat16

    far = [lax.rem(y + step, chips) for step in range(1, chips)]
    order = [yy * CORES + lax.rem(core + flip, CORES) for yy in far + [y] for flip in (1, 0)]
    early = len(order) - CORES
    offsets = list(range(1, depth)) + [0]
    targets = [
        lax.rem(z + o, depth) * SIDE + (x if flip else 1 - x) for o in offsets for flip in (0, 1)
    ]
    last = shards - 1

    p_copy = pltpu.make_async_copy(proj_hbm, pv, p_sem)
    p_copy.start()
    own_rows = pl.ds(pl.multiple_of(me * image_rows, image_rows), image_rows)
    vis_copy = pltpu.make_async_copy(vision_hbm, vv.at[own_rows], vis_sem)
    vis_copy.start()
    q_copies = [
        pltpu.make_async_copy(
            q_hbm.at[pl.ds(g * rows_dev + first, count)], dst.at[pl.ds(g * count, count)], q_sem.at[k]
        )
        for k, (first, count, dst) in enumerate(((0, per_image, q_image), (per_image, text_rows, q_text)))
        for g in range(groups)
    ]
    q_image_done = pltpu.make_async_copy(q_hbm.at[pl.ds(0, image_rows)], q_image, q_sem.at[0])
    q_text_done = pltpu.make_async_copy(q_hbm.at[pl.ds(0, groups * text_rows)], q_text, q_sem.at[1])
    w_copies = [pltpu.make_async_copy(w_hbm.at[j], wv.at[j], w_sem.at[k]) for k, j in enumerate(order)]
    gain_copy = pltpu.make_async_copy(gain_hbm, gain_ref, gain_sem)
    t_copy = pltpu.make_async_copy(text_hbm, tv, t_sem)
    for copy in q_copies[:groups] + w_copies[:1]:
        copy.start()

    barrier = pltpu.get_barrier_semaphore()
    across = z * SIDE + 1 - x
    beside = [(me, lax.rem(member + step, groups)) for step in range(1, groups)]
    beside += [(across, lax.rem(member + step, groups)) for step in range(groups)]
    for device in beside:
        pl.semaphore_signal(barrier, inc=1, device_id=device, device_id_type=MESH)

    @pl.when(z > 0)
    def _():
        pl.semaphore_signal(barrier, inc=1, device_id=(me - SIDE, member), device_id_type=MESH)

    @pl.when(z < depth - 1)
    def _():
        pl.semaphore_signal(barrier, inc=1, device_id=(me + SIDE, member), device_id_type=MESH)

    def pass_on(hop):
        @pl.when(z == hop)
        def _():
            if hop > 0:
                pl.semaphore_wait(up_sem, 1)
            if hop < depth - 1:
                pl.semaphore_signal(up_sem, inc=1, device_id=(me + SIDE, member), device_id_type=MESH)

        @pl.when(depth - 1 - z == hop)
        def _():
            if hop > 0:
                pl.semaphore_wait(down_sem, 1)
            if hop < depth - 1:
                pl.semaphore_signal(down_sem, inc=1, device_id=(me - SIDE, member), device_id_type=MESH)

    vis_copy.wait()
    for copy in w_copies[1:] + q_copies[groups:] + [gain_copy, t_copy]:
        copy.start()

    @pl.when((z == 0) | (z == depth - 1))
    def _():
        pl.semaphore_wait(barrier, len(beside) + 1)

    @pl.when((z > 0) & (z < depth - 1))
    def _():
        pl.semaphore_wait(barrier, len(beside) + 2)

    vision = VisionGather(depth, me, member, vv, image_rows, v_send, v_recv, vm_send, vm_recv)
    vision.start()
    pass_on(0)

    p_copy.wait()
    w_flat[...] = pv[...].astype(f32)
    for j in range(shards):
        w_out[j] = w_flat[pl.ds(j, shard_k, stride=fold), :].astype(bf16).T
    own_k = pl.ds(pl.multiple_of(me * shard_k, shard_k), shard_k)
    wt[:, own_k] = w_out[me]

    def w_to(t):
        j = targets[t]
        return remote(w_out.at[j], wt.at[:, own_k], wt_send, wt_recv, (j, member))

    def all_to(buf, send, recv):
        place = buf.at[pl.ds(0, last)]
        return remote(place, place, send, recv, (me, mate))

    def text_to_mate(k):
        j = order[k]
        return remote(own_text.at[j, 1 - core], mate_text.at[j], mt_send, mt_recv.at[j], (me, mate))

    def image_to_mate(yy):
        return remote(
            own_image.at[yy * CORES + 1 - core], mate_image.at[yy],
            mi_send, mi_recv.at[yy], (me, mate),
        )

    def text_to_far(k, yy):
        j = order[k]
        return remote(
            sum_text.at[j, yy], far_text.at[y, j], ft_send, ft_recv, (me, yy * CORES + core)
        )

    def piece(t):
        return pl.ds(pl.multiple_of(targets[t] * span, span), span)

    def image_to_far(yy, t):
        return remote(
            sum_image.at[yy, piece(t)], far_image.at[y, piece(t)],
            fi_send, fi_recv.at[y, t], (me, yy * CORES + core),
        )

    def image_from_far(yy, t):
        return remote(
            sum_image.at[yy, piece(t)], far_image.at[yy, piece(t)],
            fi_send, fi_recv.at[yy, t], (me, yy * CORES + core),
        )

    def image_multiply(k):
        j = order[k]
        w_copies[k].wait()

        @pl.loop(0, bc // TILE)
        def _(n):
            rows = pl.ds(pl.multiple_of(n * TILE, TILE), TILE)
            own_image[j, rows] = row_term(wv[j, rows], q_image[...]).astype(bf16)

        if k % CORES == 0:
            image_to_mate((far + [y])[k // CORES]).start()

    def text_multiply(k, part, parts):
        j = order[k]
        cols = slice(part * bc // parts, (part + 1) * bc // parts)
        term = row_term(q_text[...], wv[j, cols]).astype(bf16)
        for g in range(groups):
            own_text[j, g % CORES, g // CORES, :, cols] = term[g * text_rows : (g + 1) * text_rows]
        if part == parts - 1:
            text_to_mate(k).start()

    def add_image(yy):
        image_to_mate(yy).wait_recv()
        for t in range(shards):
            rows = piece(t)
            total = own_image[yy * CORES + core, rows].astype(f32) + mate_image[yy, rows].astype(f32)
            sum_image[yy, rows] = total.astype(bf16)
            image_to_far(yy, t).start()

    def add_text(k):
        j = order[k]
        text_to_mate(k).wait_recv()
        for yy in far:
            @pl.loop(0, text_rows // ROW_STEP)
            def _(n):
                rows = pl.ds(pl.multiple_of(n * ROW_STEP, ROW_STEP), ROW_STEP)
                total = own_text[j, core, yy, rows].astype(f32) + mate_text[j, yy, rows].astype(f32)
                sum_text[j, yy, rows] = total.astype(bf16)
            text_to_far(k, yy).start()

    lanes = lax.broadcasted_iota(jnp.int32, (span, image_rows), 1)
    slots = lax.rem(lanes, per_image)
    held = jnp.zeros((span, image_rows), jnp.int32)
    for g in range(groups):
        held = jnp.where(lanes // per_image == g, count_ref[g] * PATCH, held)
    live = slots < held

    def n_to(t):
        j = targets[t]
        return remote(n_out.at[t], nt.at[:, own_lanes], n_send, n_recv, (j, member))

    own_lanes = pl.ds(pl.multiple_of(me * image_rows, image_rows), image_rows)

    def spread_image(t):
        if t == 0:
            image_to_mate(y).wait_recv()
        for yy in far:
            image_from_far(yy, t).wait_recv()
        rows = piece(t)
        total = own_image[member, rows].astype(f32) + mate_image[y, rows].astype(f32)
        for yy in far:
            total = total + far_image[yy, rows].astype(f32)
        total = jnp.where(live, total, 0.0).astype(bf16)
        if t < last:
            n_out[t] = total
            n_to(t).start()
        else:
            nt[:, own_lanes] = total

    def each(action, *lead):
        return [functools.partial(action, *lead, chunk) for chunk in range(CHUNKS)]

    def play(*actions):
        for action in actions:
            action()

    images = [functools.partial(spread_image, t) for t in range(shards)]

    def part(k, h):
        return functools.partial(text_multiply, k, h, 2)

    def send_w(early):
        for t in range(last):
            level = targets[t] // SIDE
            near = jnp.where(z < depth // 2, level == z + 1, level == z - 1)

            @pl.when(near if early else jnp.logical_not(near))
            def _():
                w_to(t).start()

    hops = [None] + [each(vision.relay, hop) for hop in range(1, depth)]
    sides = [each(vision.side, hop) for hop in range(depth)]

    q_image_done.wait()
    for k in range(len(order)):
        image_multiply(k)
        if k + 1 < depth - 1:
            pass_on(k + 1)
        if k % CORES == 0 and k >= CORES:
            add_image(far[k // CORES - 1])
            if k == CORES:
                play(*hops[1][:1])
    for hop in range(min(len(order) + 1, depth - 1), depth):
        pass_on(hop)
    q_text_done.wait()
    play(hops[1][1], part(0, 0), hops[1][2], part(0, 1), *hops[1][3:])
    send_w(True)
    play(*sides[0])
    play(hops[2][0], part(1, 0), *hops[2][1:3], part(1, 1), *hops[2][3:])
    send_w(False)
    play(*images[:4])
    add_text(0)
    add_text(1)
    play(part(2, 0), *images[4:6], part(2, 1), *images[6:], part(3, 0), part(3, 1))
    for k in range(4, len(order)):
        play(part(k, 0), part(k, 1))
    gain_copy.wait()
    own_gain = gain_ref[:, pl.ds(pl.multiple_of(member * bc + me * span, span), span)]
    gain_t[...] = jnp.broadcast_to(own_gain, (image_rows, span)).T
    play(*sides[1])
    for hop in range(3, depth):
        for chunk in range(CHUNKS):
            play(hops[hop][chunk], sides[hop - 1][chunk])
    all_to(w_out, wt_send, wt_recv).wait_recv()

    def embed(zz):
        vision.arrive(zz)
        pair = pl.ds(pl.multiple_of(zz * SIDE * image_rows, SIDE * image_rows), SIDE * image_rows)
        rounded = row_term(wt[...], vv[pair]).astype(bf16)
        xt[:, pair] = rounded
        value = rounded.astype(f32)
        squares = jnp.sum(value * value, axis=0, keepdims=True)
        for s in range(SIDE):
            stat_f32[pl.ds(zz * SIDE + s, 1)] = squares[:, s * image_rows : (s + 1) * image_rows]

    for hop in range(depth - 2):
        vision.levels(hop, embed)
    play(*sides[depth - 1])
    for hop in range(depth - 2, depth):
        vision.levels(hop, embed)

    all_to(n_out, n_send, n_recv).wait_recv()
    for j in range(shards):
        cols = pl.ds(j * image_rows, image_rows)
        scaled = gain_t[...] * nt[:, cols].astype(f32)
        inner = jnp.sum(scaled * xt[:, cols].astype(f32), axis=0, keepdims=True)
        stat_f32[pl.ds(shards + j, 1)] = inner
    stat_own[...] = stat_f32[...].astype(bf16)

    def stat_to(k):
        device = beside[k]
        mine = lax.rem(me, SIDE) * groups + member
        return remote(stat_own, stat_near.at[mine], s_send, s_recv, device)

    near_done = pl.ds(0, len(beside))
    stat_near_done = remote(
        stat_near.at[near_done], stat_near.at[near_done], s_send, s_recv, (me, mate)
    )
    for k in range(len(beside)):
        stat_to(k).start()
    for k in range(2, len(order)):
        add_text(k)
    total = stat_f32[...]
    stat_near_done.wait_recv()
    for device in beside:
        total = total + stat_near[lax.rem(device[0], SIDE) * groups + device[1]].astype(f32)
    stat_sum[...] = total.astype(bf16)

    def line_to(o):
        target = lax.rem(z + o, depth)
        return remote(stat_sum, stat_far.at[z], z_send, z_recv, (target * SIDE + x, member))

    far_done = pl.ds(0, depth - 1)
    stat_far_done = remote(
        stat_far.at[far_done], stat_far.at[far_done], z_send, z_recv, (me, mate)
    )
    for o in range(1, depth):
        line_to(o).start()
    stat_far_done.wait_recv()
    for o in range(1, depth):
        total = total + stat_far[lax.rem(z + o, depth)].astype(f32)

    inv_all = lax.rsqrt(total[:shards] / width + norm_eps)
    pull_all = inv_all**3 * (total[shards:] / width)
    for b in range(shards):
        cols = pl.ds(b * image_rows, image_rows)
        scaled = gain_t[...] * nt[:, cols].astype(f32)
        grad = inv_all[b : b + 1] * scaled - xt[:, cols].astype(f32) * pull_all[b : b + 1]
        gt[:, cols] = grad.astype(bf16)

    def o_to(t):
        j = targets[t]
        return remote(o_out.at[j], o_in.at[me], o_send, o_recv.at[me], (j, member))

    def o_from(t):
        j = targets[t]
        return remote(o_out.at[j], o_in.at[j], o_send, o_recv.at[j], (j, member))

    out = (jnp.dot(gt[...], vv[...], preferred_element_type=f32) * grad_scale).astype(bf16)
    for j in range(shards):
        o_out[j] = out[:, j * shard_k : (j + 1) * shard_k]
    for t in range(last):
        o_to(t).start()

    text_far = sum_text.at[:, pl.ds(0, len(far))]
    text_far_done = remote(text_far, text_far, ft_send, ft_recv, (me, mate))
    text_far_done.wait_recv()
    t_copy.wait()

    @pl.loop(0, text_rows // ROW_STEP)
    def _(n):
        rows = pl.ds(pl.multiple_of(n * ROW_STEP, ROW_STEP), ROW_STEP)
        squares = jnp.zeros((ROW_STEP, 1), f32)
        inner = jnp.zeros((ROW_STEP, 1), f32)
        for j in range(groups):
            cols = pl.ds(j * bc, bc)
            x = tv[rows, cols].astype(f32)
            norm = own_text[j, core, y, rows].astype(f32) + mate_text[j, y, rows].astype(f32)
            for yy in far:
                norm = norm + far_text[yy, j, rows].astype(f32)
            scaled = gain_ref[:, cols] * norm
            squares += jnp.sum(x * x, axis=1, keepdims=True)
            inner += jnp.sum(x * scaled, axis=1, keepdims=True)
        inv = lax.rsqrt(squares / width + norm_eps)
        pull = inv**3 * (inner / width)
        for j in range(groups):
            cols = pl.ds(j * bc, bc)
            x = tv[rows, cols].astype(f32)
            norm = own_text[j, core, y, rows].astype(f32) + mate_text[j, y, rows].astype(f32)
            for yy in far:
                norm = norm + far_text[yy, j, rows].astype(f32)
            text_out[rows, cols] = (inv * (gain_ref[:, cols] * norm) - x * pull).astype(bf16)

    def finish(chunk, j):
        proj_out[pl.ds(j, shard_k, stride=fold), :] = chunk.astype(f32).T

    finish(o_out[me], me)
    for t in reversed(range(last)):
        o_from(t).wait_recv()
        finish(o_in[targets[t]], targets[t])

    vision.drain()
    all_to(w_out, wt_send, wt_recv).wait_send()
    all_to(n_out, n_send, n_recv).wait_send()
    all_to(o_out, o_send, o_recv.at[0]).wait_send()
    stat_near_done.wait_send()
    stat_far_done.wait_send()
    text_far_done.wait_send()
    remote(mate_text, mate_text, mt_send, mt_recv.at[0], (me, mate)).wait_send()
    remote(mate_image, mate_image, mi_send, mi_recv.at[0], (me, mate)).wait_send()
    image_far = sum_image.at[pl.ds(0, len(far))]
    remote(image_far, image_far, fi_send, fi_recv.at[0, 0], (me, mate)).wait_send()


def place_outputs(text_in, proj_in, text_out, proj_out, sem):
    copies = []
    for k, (src, dst) in enumerate(((text_in, text_out), (proj_in, proj_out))):
        step = src.shape[0] // PIECES
        for p in range(PIECES):
            rows = pl.ds(p * step, step)
            copies.append(pltpu.make_async_copy(src.at[rows], dst.at[rows], sem.at[k, p]))
    for copy in copies:
        copy.start()
    for copy in copies:
        copy.wait()


def live_rows(image_count, groups):
    image_rows = IMG_MAX * PATCH
    row_ids = jnp.arange(groups * image_rows, dtype=jnp.int32)
    owners = row_ids // image_rows
    slot_ids = row_ids % image_rows // PATCH
    owner_match = owners[:, None] == jnp.arange(groups, dtype=jnp.int32)[None, :]
    owner_counts = jnp.sum(jnp.where(owner_match, image_count[None, :], 0), axis=1)
    return (slot_ids < owner_counts)[:, None]


def fused_body(vision_rows, image_count, proj_flat, text_embeds, norm_gain, q_weight, q_grad):
    groups, shards = lax.axis_size("mp"), lax.axis_size("dp")
    model_width, bc = q_weight.shape
    image_rows, enc_width = vision_rows.shape
    text_rows = text_embeds.shape[0]
    shard_k = proj_flat.shape[0] * proj_flat.shape[1] // bc
    span = bc // shards
    chips, depth = groups // CORES, shards // SIDE
    all_rows = shards * image_rows
    grad_scale = 1.0 / float(all_rows) ** 0.5
    f32, bf16 = jnp.float32, jnp.bfloat16
    vmem, dma = pltpu.VMEM, pltpu.SemaphoreType.DMA
    on_chip = pl.BlockSpec(memory_space=pltpu.VMEM)
    scalars = pl.BlockSpec(memory_space=pltpu.SMEM)
    in_hbm = pl.BlockSpec(memory_space=pltpu.HBM)
    text_grad, proj_block = pl.pallas_call(
        functools.partial(kernel, shards, groups, grad_scale),
        name="projector_backward",
        out_shape=(vmem(text_embeds.shape, bf16), vmem(proj_flat.shape, f32)),
        in_specs=[scalars] + [in_hbm] * 6,
        out_specs=(on_chip, on_chip),
        scratch_shapes=[
            vmem(proj_flat.shape, bf16),
            vmem((all_rows, enc_width), bf16),
            vmem((1, model_width), f32),
            vmem((image_rows, bc), bf16),
            vmem((groups * text_rows, bc), bf16),
            vmem((groups, bc, bc), bf16),
            vmem(text_embeds.shape, bf16),
            vmem((groups, CORES, chips, text_rows, bc), bf16),
            vmem((groups, bc, image_rows), bf16),
            vmem((groups, chips, text_rows, bc), bf16),
            vmem((chips, bc, image_rows), bf16),
            vmem((groups, chips, text_rows, bc), bf16),
            vmem((chips, bc, image_rows), bf16),
            vmem((chips, groups, text_rows, bc), bf16),
            vmem((chips, bc, image_rows), bf16),
            vmem(proj_flat.shape, f32),
            vmem((shards, span, shard_k), bf16),
            vmem((span, enc_width), bf16),
            vmem((shards, span, image_rows), bf16),
            vmem((span, all_rows), bf16),
            vmem((span, all_rows), bf16),
            vmem((span, all_rows), bf16),
            vmem((span, image_rows), f32),
            vmem((shards, span, shard_k), bf16),
            vmem((shards, span, shard_k), bf16),
            vmem((2 * shards, image_rows), f32),
            vmem((2 * shards, image_rows), bf16),
            vmem((SIDE * groups, 2 * shards, image_rows), bf16),
            vmem((2 * shards, image_rows), bf16),
            vmem((depth, 2 * shards, image_rows), bf16),
            dma, dma, dma, dma((2,)), dma((groups,)), dma,
            dma((3,)), dma((shards, CHUNKS)), dma, dma((shards,)),
            dma, dma, dma, dma, dma, dma((shards,)),
            dma, dma((groups,)), dma, dma((chips,)), dma, dma, dma, dma((chips, shards)),
            dma, dma, dma, dma, pltpu.SemaphoreType.REGULAR, pltpu.SemaphoreType.REGULAR,
        ],
        compiler_params=pltpu.CompilerParams(
            collective_id=0, has_side_effects=True, vmem_limit_bytes=56 * 1024 * 1024
        ),
    )(
        image_count,
        proj_flat,
        vision_rows,
        norm_gain[None, :],
        q_grad,
        q_weight.reshape(groups, bc, bc),
        text_embeds,
    )
    kinds = (text_grad, proj_block)
    return pl.pallas_call(
        place_outputs,
        name="place_outputs",
        out_shape=tuple(jax.ShapeDtypeStruct(a.shape, a.dtype) for a in kinds),
        in_specs=[on_chip] * 2,
        out_specs=(in_hbm, in_hbm),
        scratch_shapes=[dma((2, PIECES))],
        compiler_params=pltpu.CompilerParams(vmem_limit_bytes=4 * 1024 * 1024),
    )(*kinds)


def norm_back(rows_in, grads, gain):
    inputs = rows_in.astype(jnp.float32)
    inv_rms = lax.rsqrt(jnp.mean(inputs * inputs, axis=-1, keepdims=True) + norm_eps)
    scaled = gain[None, :] * grads
    inner_mean = jnp.mean(scaled * inputs, axis=-1, keepdims=True)
    return inv_rms * scaled - inputs * inv_rms**3 * inner_mean


def general_body(vision_rows, image_count, proj_flat, text_embeds, norm_gain, q_weight, q_grad):
    groups = lax.axis_size("mp")
    member = lax.axis_index("mp")
    shards = lax.axis_size("dp")
    enc_width = vision_rows.shape[1]
    block_cols = q_weight.shape[1]
    model_width = q_weight.shape[0]
    used_count = enc_width * block_cols
    image_rows = IMG_MAX * PATCH
    gathered = lax.all_gather(proj_flat, "dp", axis=0, tiled=True)
    proj_block = gathered.reshape(-1)[:used_count].reshape(enc_width, block_cols)
    embed_cols = jnp.dot(vision_rows, proj_block, preferred_element_type=jnp.float32).astype(
        jnp.bfloat16
    )
    live_group = live_rows(image_count, groups)
    blocks = q_grad.reshape(groups, ROWS_DEV, block_cols)
    image_query = blocks[:, :image_rows].reshape(-1, block_cols)
    text_query = blocks[:, image_rows:].reshape(-1, block_cols)
    image_term = row_term(image_query, q_weight)
    image_norm = lax.psum_scatter(
        image_term.astype(jnp.bfloat16), "mp", scatter_dimension=1, tiled=True
    ).astype(jnp.float32)
    text_norm = lax.psum_scatter(
        row_term(text_query, q_weight).astype(jnp.bfloat16), "mp", scatter_dimension=0, tiled=True
    ).astype(jnp.float32)
    x_cols = embed_cols.astype(jnp.float32)
    gain_cols = lax.dynamic_slice_in_dim(norm_gain, member * block_cols, block_cols)
    scaled = gain_cols[None, :] * image_norm
    squares, inner_sum = lax.psum(
        (jnp.sum(x_cols * x_cols, axis=1), jnp.sum(scaled * x_cols, axis=1)), "mp"
    )
    inv_rms = lax.rsqrt(squares / model_width + norm_eps)[:, None]
    image_input = inv_rms * scaled - x_cols * inv_rms**3 * (inner_sum / model_width)[:, None]
    image_cols = jnp.where(live_group, image_input, 0.0).astype(jnp.bfloat16)
    text_grad = norm_back(text_embeds, text_norm, norm_gain).astype(jnp.bfloat16)
    grad_scale = 1.0 / jnp.sqrt(jnp.float32(shards * groups * image_rows))
    proj_part = (
        lax.dot_general(
            vision_rows, image_cols, (((0,), (0,)), ((), ())), preferred_element_type=jnp.float32
        )
        * grad_scale
    )
    stored_rows = proj_flat.shape[0]
    padded = jnp.pad(proj_part.reshape(-1), (0, shards * stored_rows * 128 - used_count))
    padded = padded.reshape(shards * stored_rows, 128)
    proj_grad = lax.psum_scatter(padded, "dp", scatter_dimension=0, tiled=True)
    return (text_grad, proj_grad)


def body(vision_rows, image_count, proj_flat, text_embeds, norm_gain, q_weight, q_grad):
    groups, shards = lax.axis_size("mp"), lax.axis_size("dp")
    bc = q_weight.shape[1]
    count = proj_flat.shape[0] * proj_flat.shape[1]
    shard_k = count // bc
    fits = (
        count % bc == 0
        and shard_k == LANES
        and bc == shards * LANES
        and bc % TILE == 0
        and shard_k * shards == vision_rows.shape[1]
        and shard_k == vision_rows.shape[0]
        and groups == 2 * CORES
        and groups % CORES == 0
        and vision_rows.shape[0] // groups % ROW_STEP == 0
        and text_embeds.shape[0] % (PIECES * ROW_STEP) == 0
        and shards > 2 * SIDE
        and shards % SIDE == 0
    )
    run = fused_body if fits else general_body
    return run(vision_rows, image_count, proj_flat, text_embeds, norm_gain, q_weight, q_grad)


def solution(mesh):
    return jax.shard_map(
        body,
        mesh=mesh,
        in_specs=(
            P("dp", None),
            P("dp"),
            P(("dp", "mp"), None),
            P(("dp", "mp"), None),
            P(),
            P(None, "mp"),
            P("dp", "mp"),
        ),
        out_specs=(P(("dp", "mp"), None), P(("dp", "mp"), None)),
        check_vma=False,
    )
```

```python
import functools

import jax
import jax.numpy as jnp
from jax import lax
from jax.experimental import pallas as pl
from jax.experimental.pallas import tpu as pltpu
from jax.sharding import PartitionSpec as P

IMG_MAX = 4
PATCH = 8
ROWS_DEV = 128
CORES = 2
SIDE = 2
CHUNKS = 4
PIECES = 2
LANES = 128
TILE = 512
ROW_STEP = 16

MESH = pl.DeviceIdType.MESH

norm_eps = 1e-05


def row_term(left, weight):
    return lax.dot_general(
        left, weight, (((1,), (1,)), ((), ())), preferred_element_type=jnp.float32
    )


def remote(src, dst, send, recv, device):
    return pltpu.make_async_remote_copy(
        src_ref=src, dst_ref=dst, send_sem=send, recv_sem=recv,
        device_id=device, device_id_type=MESH,
    )


class VisionGather:
    def __init__(self, depth, me, member, buf, block_rows, send, recv, mate_send, mate_recv):
        self.depth, self.me, self.member = depth, me, member
        self.z, self.x = me // SIDE, me % SIDE
        self.core = member % CORES
        self.mate = member + 1 - 2 * self.core
        self.buf, self.block_rows = buf, block_rows
        self.send, self.recv = send, recv
        self.mate_send, self.mate_recv = mate_send, mate_recv
        self.half = block_rows // CORES
        self.step = self.half // CHUNKS

    def place(self, block, chunk, core):
        first = block * self.block_rows + core * self.half + chunk * self.step
        return self.buf.at[pl.ds(pl.multiple_of(first, self.step), self.step)]

    def copy(self, zz, x, chunk, way):
        block = zz * SIDE + x
        place = self.place(block, chunk, self.core)
        target = (self.me + SIDE, self.me - SIDE, self.z * SIDE + 1 - self.x)[way]
        return remote(
            place, place, self.send.at[way], self.recv.at[block, chunk],
            (target, self.member),
        )

    def to_mate(self, block, chunk):
        place = self.place(block, chunk, self.core)
        return remote(
            place, place, self.mate_send, self.mate_recv.at[block],
            (self.me, self.mate),
        )

    def from_mate(self, block):
        first = block * self.block_rows + (1 - self.core) * self.half
        place = self.buf.at[pl.ds(pl.multiple_of(first, self.half), self.half)]
        return remote(place, place, self.mate_send, self.mate_recv.at[block], (self.me, self.mate))

    def sent(self, send, blocks):
        place = self.buf.at[pl.ds(0, blocks * self.half)]
        remote(place, place, send, self.mate_recv.at[0], (self.me, self.mate)).wait_send()

    def start(self):
        for chunk in range(CHUNKS):
            @pl.when(self.z < self.depth - 1)
            def _():
                self.copy(self.z, self.x, chunk, 0).start()

            @pl.when(self.z > 0)
            def _():
                self.copy(self.z, self.x, chunk, 1).start()

            self.copy(self.z, self.x, chunk, 2).start()

    def relay(self, hop, chunk):
        below, above = self.z - hop, self.z + hop

        @pl.when(below >= 0)
        def _():
            self.copy(below, self.x, chunk, 0).wait_recv()

            @pl.when(self.z < self.depth - 1)
            def _():
                self.copy(below, self.x, chunk, 0).start()

            self.copy(below, self.x, chunk, 2).start()
            self.to_mate(below * SIDE + self.x, chunk).start()

        @pl.when(above < self.depth)
        def _():
            self.copy(above, self.x, chunk, 1).wait_recv()

            @pl.when(self.z > 0)
            def _():
                self.copy(above, self.x, chunk, 1).start()

            self.copy(above, self.x, chunk, 2).start()
            self.to_mate(above * SIDE + self.x, chunk).start()

    def levels(self, hop, use):
        for zz in (self.z,) if hop == 0 else (self.z - hop, self.z + hop):
            @pl.when((zz >= 0) & (zz < self.depth))
            def _():
                use(zz)

    def side(self, hop, chunk):
        def take(zz):
            self.copy(zz, 1 - self.x, chunk, 2).wait_recv()
            self.to_mate(zz * SIDE + 1 - self.x, chunk).start()

        self.levels(hop, take)

    def arrive(self, zz):
        @pl.when(zz != self.z)
        def _():
            self.from_mate(zz * SIDE + self.x).wait_recv()

        self.from_mate(zz * SIDE + 1 - self.x).wait_recv()

    def drain(self):
        for zz in range(self.depth):
            @pl.when(self.z == zz)
            def _():
                if zz < self.depth - 1:
                    self.sent(self.send.at[0], zz + 1)
                if zz > 0:
                    self.sent(self.send.at[1], self.depth - zz)
        self.sent(self.send.at[2], self.depth)
        self.sent(self.mate_send, SIDE * self.depth - 1)


def kernel(
    shards, groups, grad_scale,
    count_ref, proj_hbm, vision_hbm, gain_hbm, q_hbm, w_hbm, text_hbm,
    text_out, proj_out,
    pv, vv, gain_ref, q_image, q_text, wv, tv,
    own_text, own_image, mate_text, mate_image, sum_text, sum_image,
    far_text, far_image, w_flat, w_out, wt, n_out, nt, xt, gt, gain_t, o_out, o_in,
    stat_f32, stat_own, stat_near, stat_sum, stat_far,
    p_sem, vis_sem, gain_sem, q_sem, w_sem, t_sem,
    v_send, v_recv, vm_send, vm_recv, wt_send, wt_recv, n_send, n_recv, o_send, o_recv,
    mt_send, mt_recv, mi_send, mi_recv, ft_send, ft_recv, fi_send, fi_recv,
    s_send, s_recv, z_send, z_recv, up_sem, down_sem,
):
    me, member = lax.axis_index("dp"), lax.axis_index("mp")
    depth = shards // SIDE
    chips = groups // CORES
    y, core = member // CORES, member % CORES
    mate = y * CORES + 1 - core
    z, x = me // SIDE, me % SIDE
    bc = wv.shape[1]
    span = bc // shards
    fold = bc // LANES
    shard_k = wt.shape[1] // shards
    image_rows = q_image.shape[0]
    per_image = image_rows // groups
    text_rows = tv.shape[0]
    rows_dev = per_image + text_rows
    width = groups * bc
    f32, bf16 = jnp.float32, jnp.bfloat16

    far = [lax.rem(y + step, chips) for step in range(1, chips)]
    order = [yy * CORES + lax.rem(core + flip, CORES) for yy in far + [y] for flip in (1, 0)]
    early = len(order) - CORES
    offsets = list(range(1, depth)) + [0]
    targets = [
        lax.rem(z + o, depth) * SIDE + (x if flip else 1 - x) for o in offsets for flip in (0, 1)
    ]
    last = shards - 1

    barrier = pltpu.get_barrier_semaphore()
    across = z * SIDE + 1 - x
    beside = [(me, lax.rem(member + step, groups)) for step in range(1, groups)]
    beside += [(across, lax.rem(member + step, groups)) for step in range(groups)]
    greeted = beside[: groups - 1] + [(across, member)]
    for device in greeted:
        pl.semaphore_signal(barrier, inc=1, device_id=device, device_id_type=MESH)

    @pl.when(z > 0)
    def _():
        pl.semaphore_signal(barrier, inc=1, device_id=(me - SIDE, member), device_id_type=MESH)

    @pl.when(z < depth - 1)
    def _():
        pl.semaphore_signal(barrier, inc=1, device_id=(me + SIDE, member), device_id_type=MESH)

    own_rows = pl.ds(pl.multiple_of(me * image_rows, image_rows), image_rows)
    vis_copy = pltpu.make_async_copy(vision_hbm, vv.at[own_rows], vis_sem)
    vis_copy.start()
    p_copy = pltpu.make_async_copy(proj_hbm, pv, p_sem)
    p_copy.start()
    q_copies = [
        pltpu.make_async_copy(
            q_hbm.at[pl.ds(g * rows_dev + first, count)], dst.at[pl.ds(g * count, count)], q_sem.at[k]
        )
        for k, (first, count, dst) in enumerate(((0, per_image, q_image), (per_image, text_rows, q_text)))
        for g in range(groups)
    ]
    q_image_done = pltpu.make_async_copy(q_hbm.at[pl.ds(0, image_rows)], q_image, q_sem.at[0])
    q_text_done = pltpu.make_async_copy(q_hbm.at[pl.ds(0, groups * text_rows)], q_text, q_sem.at[1])
    w_copies = [pltpu.make_async_copy(w_hbm.at[j], wv.at[j], w_sem.at[k]) for k, j in enumerate(order)]
    gain_copy = pltpu.make_async_copy(gain_hbm, gain_ref, gain_sem)
    t_copy = pltpu.make_async_copy(text_hbm, tv, t_sem)
    for copy in q_copies[:groups] + w_copies[:1]:
        copy.start()

    def pass_on(hop):
        @pl.when(z == hop)
        def _():
            if hop > 0:
                pl.semaphore_wait(up_sem, 1)
            if hop < depth - 1:
                pl.semaphore_signal(up_sem, inc=1, device_id=(me + SIDE, member), device_id_type=MESH)

        @pl.when(depth - 1 - z == hop)
        def _():
            if hop > 0:
                pl.semaphore_wait(down_sem, 1)
            if hop < depth - 1:
                pl.semaphore_signal(down_sem, inc=1, device_id=(me - SIDE, member), device_id_type=MESH)

    vis_copy.wait()
    for copy in w_copies[1:] + q_copies[groups:] + [gain_copy, t_copy]:
        copy.start()

    @pl.when((z == 0) | (z == depth - 1))
    def _():
        pl.semaphore_wait(barrier, len(greeted) + 1)

    @pl.when((z > 0) & (z < depth - 1))
    def _():
        pl.semaphore_wait(barrier, len(greeted) + 2)

    vision = VisionGather(depth, me, member, vv, image_rows, v_send, v_recv, vm_send, vm_recv)
    vision.start()
    pass_on(0)

    p_copy.wait()
    w_flat[...] = pv[...].astype(f32)
    for j in range(shards):
        w_out[j] = w_flat[pl.ds(j, shard_k, stride=fold), :].astype(bf16).T
    own_k = pl.ds(pl.multiple_of(me * shard_k, shard_k), shard_k)
    wt[:, own_k] = w_out[me]

    def w_to(t):
        j = targets[t]
        return remote(w_out.at[j], wt.at[:, own_k], wt_send, wt_recv, (j, member))

    def all_to(buf, send, recv):
        place = buf.at[pl.ds(0, last)]
        return remote(place, place, send, recv, (me, mate))

    def send_w(stage):
        for t in range(last):
            level = targets[t] // SIDE
            outward = jnp.where(z < depth // 2, z + 1, z - 1)
            straight = (level == z) | ((level - z) * (level - z) == 1) & (targets[t] % SIDE == x)
            aside = jnp.logical_not(straight) & (level == outward)
            due = (straight, aside, jnp.logical_not(straight | aside))[stage]

            @pl.when(due)
            def _():
                w_to(t).start()

    send_w(0)

    def text_to_mate(k):
        j = order[k]
        return remote(own_text.at[j, 1 - core], mate_text.at[j], mt_send, mt_recv.at[j], (me, mate))

    def image_to_mate(yy):
        return remote(
            own_image.at[yy * CORES + 1 - core], mate_image.at[yy],
            mi_send, mi_recv.at[yy], (me, mate),
        )

    def text_to_far(k, yy):
        j = order[k]
        return remote(
            sum_text.at[j, yy], far_text.at[y, j], ft_send, ft_recv, (me, yy * CORES + core)
        )

    def piece(t):
        return pl.ds(pl.multiple_of(targets[t] * span, span), span)

    def image_to_far(yy, t):
        return remote(
            sum_image.at[yy, piece(t)], far_image.at[y, piece(t)],
            fi_send, fi_recv.at[t], (me, yy * CORES + core),
        )

    def image_from_far(yy, t):
        return remote(
            sum_image.at[yy, piece(t)], far_image.at[yy, piece(t)],
            fi_send, fi_recv.at[t], (me, yy * CORES + core),
        )

    def image_multiply(k):
        j = order[k]
        w_copies[k].wait()

        @pl.loop(0, bc // TILE)
        def _(n):
            rows = pl.ds(pl.multiple_of(n * TILE, TILE), TILE)
            own_image[j, rows] = row_term(wv[j, rows], q_image[...]).astype(bf16)

        if k % CORES == 0:
            image_to_mate((far + [y])[k // CORES]).start()

    def text_multiply(k, part, parts):
        j = order[k]
        cols = slice(part * bc // parts, (part + 1) * bc // parts)
        term = row_term(q_text[...], wv[j, cols]).astype(bf16)
        for g in range(groups):
            own_text[j, g % CORES, g // CORES, :, cols] = term[g * text_rows : (g + 1) * text_rows]
        if part == parts - 1:
            text_to_mate(k).start()

    def add_image(yy):
        image_to_mate(yy).wait_recv()
        for t in range(shards):
            rows = piece(t)
            total = own_image[yy * CORES + core, rows].astype(f32) + mate_image[yy, rows].astype(f32)
            sum_image[yy, rows] = total.astype(bf16)
            image_to_far(yy, t).start()

    def add_text(k):
        j = order[k]
        text_to_mate(k).wait_recv()
        for yy in far:
            @pl.loop(0, text_rows // ROW_STEP)
            def _(n):
                rows = pl.ds(pl.multiple_of(n * ROW_STEP, ROW_STEP), ROW_STEP)
                total = own_text[j, core, yy, rows].astype(f32) + mate_text[j, yy, rows].astype(f32)
                sum_text[j, yy, rows] = total.astype(bf16)
            text_to_far(k, yy).start()

    lanes = lax.broadcasted_iota(jnp.int32, (span, image_rows), 1)
    slots = lax.rem(lanes, per_image)
    held = jnp.zeros((span, image_rows), jnp.int32)
    for g in range(groups):
        held = jnp.where(lanes // per_image == g, count_ref[g] * PATCH, held)
    live = slots < held

    def n_to(t):
        j = targets[t]
        return remote(n_out.at[t], nt.at[:, own_lanes], n_send, n_recv, (j, member))

    own_lanes = pl.ds(pl.multiple_of(me * image_rows, image_rows), image_rows)

    def spread_image(t):
        if t == 0:
            image_to_mate(y).wait_recv()
        for yy in far:
            image_from_far(yy, t).wait_recv()
        rows = piece(t)
        total = own_image[member, rows].astype(f32) + mate_image[y, rows].astype(f32)
        for yy in far:
            total = total + far_image[yy, rows].astype(f32)
        total = jnp.where(live, total, 0.0).astype(bf16)
        if t < last:
            n_out[t] = total
            n_to(t).start()
        else:
            nt[:, own_lanes] = total

    def each(action, *lead):
        return [functools.partial(action, *lead, chunk) for chunk in range(CHUNKS)]

    def play(*actions):
        for action in actions:
            action()

    images = [functools.partial(spread_image, t) for t in range(shards)]

    def part(k, h):
        return functools.partial(text_multiply, k, h, 2)

    hops = [None] + [each(vision.relay, hop) for hop in range(1, depth)]
    sides = [each(vision.side, hop) for hop in range(depth)]

    q_image_done.wait()
    for k in range(len(order)):
        image_multiply(k)
        if k + 1 < depth - 1:
            pass_on(k + 1)
        if k % CORES == 0 and k >= CORES:
            add_image(far[k // CORES - 1])
            if k == CORES:
                play(*hops[1][:1])
    for hop in range(min(len(order) + 1, depth - 1), depth):
        pass_on(hop)
    q_text_done.wait()
    play(hops[1][1], part(0, 0), hops[1][2], part(0, 1), *hops[1][3:])
    send_w(1)
    play(*sides[0])
    play(hops[2][0], part(1, 0), *hops[2][1:3], part(1, 1), *hops[2][3:])
    send_w(2)
    play(*images[:4])
    add_text(0)
    add_text(1)
    play(part(2, 0), *images[4:6], part(2, 1), *images[6:], part(3, 0), part(3, 1))
    for k in range(4, len(order)):
        play(part(k, 0), part(k, 1))
    gain_copy.wait()
    own_gain = gain_ref[:, pl.ds(pl.multiple_of(member * bc + me * span, span), span)]
    gain_t[...] = jnp.broadcast_to(own_gain, (image_rows, span)).T
    play(*sides[1])
    for hop in range(3, depth):
        for chunk in range(CHUNKS):
            play(hops[hop][chunk], sides[hop - 1][chunk])
    all_to(w_out, wt_send, wt_recv).wait_recv()

    def embed(zz):
        vision.arrive(zz)
        pair = pl.ds(pl.multiple_of(zz * SIDE * image_rows, SIDE * image_rows), SIDE * image_rows)
        rounded = row_term(wt[...], vv[pair]).astype(bf16)
        xt[:, pair] = rounded
        value = rounded.astype(f32)
        squares = jnp.sum(value * value, axis=0, keepdims=True)
        for s in range(SIDE):
            stat_f32[pl.ds(zz * SIDE + s, 1)] = squares[:, s * image_rows : (s + 1) * image_rows]

    for hop in range(depth - 2):
        vision.levels(hop, embed)
    play(*sides[depth - 1])
    for hop in range(depth - 2, depth):
        vision.levels(hop, embed)

    all_to(n_out, n_send, n_recv).wait_recv()
    for j in range(shards):
        cols = pl.ds(j * image_rows, image_rows)
        scaled = gain_t[...] * nt[:, cols].astype(f32)
        inner = jnp.sum(scaled * xt[:, cols].astype(f32), axis=0, keepdims=True)
        stat_f32[pl.ds(shards + j, 1)] = inner
    stat_own[...] = stat_f32[...].astype(bf16)

    def stat_to(k):
        device = beside[k]
        mine = lax.rem(me, SIDE) * groups + member
        return remote(stat_own, stat_near.at[mine], s_send, s_recv, device)

    near_done = pl.ds(0, len(beside))
    stat_near_done = remote(
        stat_near.at[near_done], stat_near.at[near_done], s_send, s_recv, (me, mate)
    )
    for k in range(len(beside)):
        stat_to(k).start()
    for k in range(2, len(order)):
        add_text(k)
    total = stat_f32[...]
    stat_near_done.wait_recv()
    for device in beside:
        total = total + stat_near[lax.rem(device[0], SIDE) * groups + device[1]].astype(f32)
    stat_sum[...] = total.astype(bf16)

    def line_to(o):
        target = lax.rem(z + o, depth)
        return remote(stat_sum, stat_far.at[z], z_send, z_recv, (target * SIDE + x, member))

    far_done = pl.ds(0, depth - 1)
    stat_far_done = remote(
        stat_far.at[far_done], stat_far.at[far_done], z_send, z_recv, (me, mate)
    )
    for o in range(1, depth):
        line_to(o).start()
    stat_far_done.wait_recv()
    for o in range(1, depth):
        total = total + stat_far[lax.rem(z + o, depth)].astype(f32)

    inv_all = lax.rsqrt(total[:shards] / width + norm_eps)
    pull_all = inv_all**3 * (total[shards:] / width)
    for b in range(shards):
        cols = pl.ds(b * image_rows, image_rows)
        scaled = gain_t[...] * nt[:, cols].astype(f32)
        grad = inv_all[b : b + 1] * scaled - xt[:, cols].astype(f32) * pull_all[b : b + 1]
        gt[:, cols] = grad.astype(bf16)

    def o_to(t):
        j = targets[t]
        return remote(o_out.at[j], o_in.at[me], o_send, o_recv.at[me], (j, member))

    def o_from(t):
        j = targets[t]
        return remote(o_out.at[j], o_in.at[j], o_send, o_recv.at[j], (j, member))

    out = (jnp.dot(gt[...], vv[...], preferred_element_type=f32) * grad_scale).astype(bf16)
    for j in range(shards):
        o_out[j] = out[:, j * shard_k : (j + 1) * shard_k]
    for t in range(last):
        o_to(t).start()

    text_far = sum_text.at[:, pl.ds(0, len(far))]
    text_far_done = remote(text_far, text_far, ft_send, ft_recv, (me, mate))
    text_far_done.wait_recv()
    t_copy.wait()

    @pl.loop(0, text_rows // ROW_STEP)
    def _(n):
        rows = pl.ds(pl.multiple_of(n * ROW_STEP, ROW_STEP), ROW_STEP)
        squares = jnp.zeros((ROW_STEP, 1), f32)
        inner = jnp.zeros((ROW_STEP, 1), f32)
        for j in range(groups):
            cols = pl.ds(j * bc, bc)
            x = tv[rows, cols].astype(f32)
            norm = own_text[j, core, y, rows].astype(f32) + mate_text[j, y, rows].astype(f32)
            for yy in far:
                norm = norm + far_text[yy, j, rows].astype(f32)
            scaled = gain_ref[:, cols] * norm
            squares += jnp.sum(x * x, axis=1, keepdims=True)
            inner += jnp.sum(x * scaled, axis=1, keepdims=True)
        inv = lax.rsqrt(squares / width + norm_eps)
        pull = inv**3 * (inner / width)
        for j in range(groups):
            cols = pl.ds(j * bc, bc)
            x = tv[rows, cols].astype(f32)
            norm = own_text[j, core, y, rows].astype(f32) + mate_text[j, y, rows].astype(f32)
            for yy in far:
                norm = norm + far_text[yy, j, rows].astype(f32)
            text_out[rows, cols] = (inv * (gain_ref[:, cols] * norm) - x * pull).astype(bf16)

    def finish(chunk, j):
        proj_out[pl.ds(j, shard_k, stride=fold), :] = chunk.astype(f32).T

    finish(o_out[me], me)
    for t in reversed(range(last)):
        o_from(t).wait_recv()
        finish(o_in[targets[t]], targets[t])

    vision.drain()
    all_to(w_out, wt_send, wt_recv).wait_send()
    all_to(n_out, n_send, n_recv).wait_send()
    all_to(o_out, o_send, o_recv.at[0]).wait_send()
    stat_near_done.wait_send()
    stat_far_done.wait_send()
    text_far_done.wait_send()
    remote(mate_text, mate_text, mt_send, mt_recv.at[0], (me, mate)).wait_send()
    remote(mate_image, mate_image, mi_send, mi_recv.at[0], (me, mate)).wait_send()
    image_far = sum_image.at[pl.ds(0, len(far))]
    remote(image_far, image_far, fi_send, fi_recv.at[0], (me, mate)).wait_send()


def place_outputs(text_in, proj_in, text_out, proj_out, sem):
    copies = []
    for k, (src, dst) in enumerate(((text_in, text_out), (proj_in, proj_out))):
        step = src.shape[0] // PIECES
        for p in range(PIECES):
            rows = pl.ds(p * step, step)
            copies.append(pltpu.make_async_copy(src.at[rows], dst.at[rows], sem.at[k, p]))
    for copy in copies:
        copy.start()
    for copy in copies:
        copy.wait()


def live_rows(image_count, groups):
    image_rows = IMG_MAX * PATCH
    row_ids = jnp.arange(groups * image_rows, dtype=jnp.int32)
    owners = row_ids // image_rows
    slot_ids = row_ids % image_rows // PATCH
    owner_match = owners[:, None] == jnp.arange(groups, dtype=jnp.int32)[None, :]
    owner_counts = jnp.sum(jnp.where(owner_match, image_count[None, :], 0), axis=1)
    return (slot_ids < owner_counts)[:, None]


def fused_body(vision_rows, image_count, proj_flat, text_embeds, norm_gain, q_weight, q_grad):
    groups, shards = lax.axis_size("mp"), lax.axis_size("dp")
    model_width, bc = q_weight.shape
    image_rows, enc_width = vision_rows.shape
    text_rows = text_embeds.shape[0]
    shard_k = proj_flat.shape[0] * proj_flat.shape[1] // bc
    span = bc // shards
    chips, depth = groups // CORES, shards // SIDE
    all_rows = shards * image_rows
    grad_scale = 1.0 / float(all_rows) ** 0.5
    f32, bf16 = jnp.float32, jnp.bfloat16
    vmem, dma = pltpu.VMEM, pltpu.SemaphoreType.DMA
    on_chip = pl.BlockSpec(memory_space=pltpu.VMEM)
    scalars = pl.BlockSpec(memory_space=pltpu.SMEM)
    in_hbm = pl.BlockSpec(memory_space=pltpu.HBM)
    text_grad, proj_block = pl.pallas_call(
        functools.partial(kernel, shards, groups, grad_scale),
        name="projector_backward",
        out_shape=(vmem(text_embeds.shape, bf16), vmem(proj_flat.shape, f32)),
        in_specs=[scalars] + [in_hbm] * 6,
        out_specs=(on_chip, on_chip),
        scratch_shapes=[
            vmem(proj_flat.shape, bf16),
            vmem((all_rows, enc_width), bf16),
            vmem((1, model_width), f32),
            vmem((image_rows, bc), bf16),
            vmem((groups * text_rows, bc), bf16),
            vmem((groups, bc, bc), bf16),
            vmem(text_embeds.shape, bf16),
            vmem((groups, CORES, chips, text_rows, bc), bf16),
            vmem((groups, bc, image_rows), bf16),
            vmem((groups, chips, text_rows, bc), bf16),
            vmem((chips, bc, image_rows), bf16),
            vmem((groups, chips, text_rows, bc), bf16),
            vmem((chips, bc, image_rows), bf16),
            vmem((chips, groups, text_rows, bc), bf16),
            vmem((chips, bc, image_rows), bf16),
            vmem(proj_flat.shape, f32),
            vmem((shards, span, shard_k), bf16),
            vmem((span, enc_width), bf16),
            vmem((shards, span, image_rows), bf16),
            vmem((span, all_rows), bf16),
            vmem((span, all_rows), bf16),
            vmem((span, all_rows), bf16),
            vmem((span, image_rows), f32),
            vmem((shards, span, shard_k), bf16),
            vmem((shards, span, shard_k), bf16),
            vmem((2 * shards, image_rows), f32),
            vmem((2 * shards, image_rows), bf16),
            vmem((SIDE * groups, 2 * shards, image_rows), bf16),
            vmem((2 * shards, image_rows), bf16),
            vmem((depth, 2 * shards, image_rows), bf16),
            dma, dma, dma, dma((2,)), dma((groups,)), dma,
            dma((3,)), dma((shards, CHUNKS)), dma, dma((shards,)),
            dma, dma, dma, dma, dma, dma((shards,)),
            dma, dma((groups,)), dma, dma((chips,)), dma, dma, dma, dma((shards,)),
            dma, dma, dma, dma, pltpu.SemaphoreType.REGULAR, pltpu.SemaphoreType.REGULAR,
        ],
        compiler_params=pltpu.CompilerParams(
            collective_id=0, has_side_effects=True, vmem_limit_bytes=56 * 1024 * 1024
        ),
    )(
        image_count,
        proj_flat,
        vision_rows,
        norm_gain[None, :],
        q_grad,
        q_weight.reshape(groups, bc, bc),
        text_embeds,
    )
    kinds = (text_grad, proj_block)
    return pl.pallas_call(
        place_outputs,
        name="place_outputs",
        out_shape=tuple(jax.ShapeDtypeStruct(a.shape, a.dtype) for a in kinds),
        in_specs=[on_chip] * 2,
        out_specs=(in_hbm, in_hbm),
        scratch_shapes=[dma((2, PIECES))],
        compiler_params=pltpu.CompilerParams(vmem_limit_bytes=4 * 1024 * 1024),
    )(*kinds)


def norm_back(rows_in, grads, gain):
    inputs = rows_in.astype(jnp.float32)
    inv_rms = lax.rsqrt(jnp.mean(inputs * inputs, axis=-1, keepdims=True) + norm_eps)
    scaled = gain[None, :] * grads
    inner_mean = jnp.mean(scaled * inputs, axis=-1, keepdims=True)
    return inv_rms * scaled - inputs * inv_rms**3 * inner_mean


def general_body(vision_rows, image_count, proj_flat, text_embeds, norm_gain, q_weight, q_grad):
    groups = lax.axis_size("mp")
    member = lax.axis_index("mp")
    shards = lax.axis_size("dp")
    enc_width = vision_rows.shape[1]
    block_cols = q_weight.shape[1]
    model_width = q_weight.shape[0]
    used_count = enc_width * block_cols
    image_rows = IMG_MAX * PATCH
    gathered = lax.all_gather(proj_flat, "dp", axis=0, tiled=True)
    proj_block = gathered.reshape(-1)[:used_count].reshape(enc_width, block_cols)
    embed_cols = jnp.dot(vision_rows, proj_block, preferred_element_type=jnp.float32).astype(
        jnp.bfloat16
    )
    live_group = live_rows(image_count, groups)
    blocks = q_grad.reshape(groups, ROWS_DEV, block_cols)
    image_query = blocks[:, :image_rows].reshape(-1, block_cols)
    text_query = blocks[:, image_rows:].reshape(-1, block_cols)
    image_term = row_term(image_query, q_weight)
    image_norm = lax.psum_scatter(
        image_term.astype(jnp.bfloat16), "mp", scatter_dimension=1, tiled=True
    ).astype(jnp.float32)
    text_norm = lax.psum_scatter(
        row_term(text_query, q_weight).astype(jnp.bfloat16), "mp", scatter_dimension=0, tiled=True
    ).astype(jnp.float32)
    x_cols = embed_cols.astype(jnp.float32)
    gain_cols = lax.dynamic_slice_in_dim(norm_gain, member * block_cols, block_cols)
    scaled = gain_cols[None, :] * image_norm
    squares, inner_sum = lax.psum(
        (jnp.sum(x_cols * x_cols, axis=1), jnp.sum(scaled * x_cols, axis=1)), "mp"
    )
    inv_rms = lax.rsqrt(squares / model_width + norm_eps)[:, None]
    image_input = inv_rms * scaled - x_cols * inv_rms**3 * (inner_sum / model_width)[:, None]
    image_cols = jnp.where(live_group, image_input, 0.0).astype(jnp.bfloat16)
    text_grad = norm_back(text_embeds, text_norm, norm_gain).astype(jnp.bfloat16)
    grad_scale = 1.0 / jnp.sqrt(jnp.float32(shards * groups * image_rows))
    proj_part = (
        lax.dot_general(
            vision_rows, image_cols, (((0,), (0,)), ((), ())), preferred_element_type=jnp.float32
        )
        * grad_scale
    )
    stored_rows = proj_flat.shape[0]
    padded = jnp.pad(proj_part.reshape(-1), (0, shards * stored_rows * 128 - used_count))
    padded = padded.reshape(shards * stored_rows, 128)
    proj_grad = lax.psum_scatter(padded, "dp", scatter_dimension=0, tiled=True)
    return (text_grad, proj_grad)


def body(vision_rows, image_count, proj_flat, text_embeds, norm_gain, q_weight, q_grad):
    groups, shards = lax.axis_size("mp"), lax.axis_size("dp")
    bc = q_weight.shape[1]
    count = proj_flat.shape[0] * proj_flat.shape[1]
    shard_k = count // bc
    fits = (
        count % bc == 0
        and shard_k == LANES
        and bc == shards * LANES
        and bc % TILE == 0
        and shard_k * shards == vision_rows.shape[1]
        and shard_k == vision_rows.shape[0]
        and groups == 2 * CORES
        and groups % CORES == 0
        and vision_rows.shape[0] // groups % ROW_STEP == 0
        and text_embeds.shape[0] % (PIECES * ROW_STEP) == 0
        and shards > 2 * SIDE
        and shards % SIDE == 0
    )
    run = fused_body if fits else general_body
    return run(vision_rows, image_count, proj_flat, text_embeds, norm_gain, q_weight, q_grad)


def solution(mesh):
    return jax.shard_map(
        body,
        mesh=mesh,
        in_specs=(
            P("dp", None),
            P("dp"),
            P(("dp", "mp"), None),
            P(("dp", "mp"), None),
            P(),
            P(None, "mp"),
            P("dp", "mp"),
        ),
        out_specs=(P(("dp", "mp"), None), P(("dp", "mp"), None)),
        check_vma=False,
    )
```

```python
import functools

import jax
import jax.numpy as jnp
from jax import lax
from jax.experimental import pallas as pl
from jax.experimental.pallas import tpu as pltpu
from jax.sharding import PartitionSpec as P

IMG_MAX = 4
PATCH = 8
ROWS_DEV = 128
CORES = 2
SIDE = 2
CHUNKS = 4
PIECES = 2
LANES = 128
TILE = 512
ROW_STEP = 16

MESH = pl.DeviceIdType.MESH

norm_eps = 1e-05


def row_term(left, weight):
    return lax.dot_general(
        left, weight, (((1,), (1,)), ((), ())), preferred_element_type=jnp.float32
    )


def remote(src, dst, send, recv, device):
    return pltpu.make_async_remote_copy(
        src_ref=src, dst_ref=dst, send_sem=send, recv_sem=recv,
        device_id=device, device_id_type=MESH,
    )


class VisionGather:
    def __init__(self, depth, me, member, buf, block_rows, send, recv, mate_send, mate_recv):
        self.depth, self.me, self.member = depth, me, member
        self.z, self.x = me // SIDE, me % SIDE
        self.core = member % CORES
        self.mate = member + 1 - 2 * self.core
        self.buf, self.block_rows = buf, block_rows
        self.send, self.recv = send, recv
        self.mate_send, self.mate_recv = mate_send, mate_recv
        self.half = block_rows // CORES
        self.step = self.half // CHUNKS

    def place(self, block, chunk, core):
        first = block * self.block_rows + core * self.half + chunk * self.step
        return self.buf.at[pl.ds(pl.multiple_of(first, self.step), self.step)]

    def copy(self, zz, x, chunk, way):
        block = zz * SIDE + x
        place = self.place(block, chunk, self.core)
        target = (self.me + SIDE, self.me - SIDE, self.z * SIDE + 1 - self.x)[way]
        return remote(
            place, place, self.send.at[way], self.recv.at[block, chunk],
            (target, self.member),
        )

    def to_mate(self, block, chunk):
        place = self.place(block, chunk, self.core)
        return remote(
            place, place, self.mate_send, self.mate_recv.at[block],
            (self.me, self.mate),
        )

    def from_mate(self, block):
        first = block * self.block_rows + (1 - self.core) * self.half
        place = self.buf.at[pl.ds(pl.multiple_of(first, self.half), self.half)]
        return remote(place, place, self.mate_send, self.mate_recv.at[block], (self.me, self.mate))

    def sent(self, send, blocks):
        place = self.buf.at[pl.ds(0, blocks * self.half)]
        remote(place, place, send, self.mate_recv.at[0], (self.me, self.mate)).wait_send()

    def start(self):
        for chunk in range(CHUNKS):
            @pl.when(self.z < self.depth - 1)
            def _():
                self.copy(self.z, self.x, chunk, 0).start()

            @pl.when(self.z > 0)
            def _():
                self.copy(self.z, self.x, chunk, 1).start()

            self.copy(self.z, self.x, chunk, 2).start()

    def relay(self, hop, chunk):
        below, above = self.z - hop, self.z + hop

        @pl.when(below >= 0)
        def _():
            self.copy(below, self.x, chunk, 0).wait_recv()

            @pl.when(self.z < self.depth - 1)
            def _():
                self.copy(below, self.x, chunk, 0).start()

            self.copy(below, self.x, chunk, 2).start()
            self.to_mate(below * SIDE + self.x, chunk).start()

        @pl.when(above < self.depth)
        def _():
            self.copy(above, self.x, chunk, 1).wait_recv()

            @pl.when(self.z > 0)
            def _():
                self.copy(above, self.x, chunk, 1).start()

            self.copy(above, self.x, chunk, 2).start()
            self.to_mate(above * SIDE + self.x, chunk).start()

    def levels(self, hop, use):
        for zz in (self.z,) if hop == 0 else (self.z - hop, self.z + hop):
            @pl.when((zz >= 0) & (zz < self.depth))
            def _():
                use(zz)

    def side(self, hop, chunk):
        def take(zz):
            self.copy(zz, 1 - self.x, chunk, 2).wait_recv()
            self.to_mate(zz * SIDE + 1 - self.x, chunk).start()

        self.levels(hop, take)

    def arrive(self, zz):
        @pl.when(zz != self.z)
        def _():
            self.from_mate(zz * SIDE + self.x).wait_recv()

        self.from_mate(zz * SIDE + 1 - self.x).wait_recv()

    def drain(self):
        for zz in range(self.depth):
            @pl.when(self.z == zz)
            def _():
                if zz < self.depth - 1:
                    self.sent(self.send.at[0], zz + 1)
                if zz > 0:
                    self.sent(self.send.at[1], self.depth - zz)
        self.sent(self.send.at[2], self.depth)
        self.sent(self.mate_send, SIDE * self.depth - 1)


def kernel(
    shards, groups, grad_scale,
    count_ref, proj_hbm, vision_hbm, gain_hbm, q_hbm, w_hbm, text_hbm,
    text_out, proj_out,
    pv, vv, gain_ref, q_image, q_text, wv, tv,
    own_text, own_image, mate_text, mate_image, sum_text, sum_image,
    far_text, far_image, w_flat, w_out, wt, n_out, nt, xt, gt, gain_t, o_out, o_in,
    stat_f32, stat_own, stat_near, stat_sum, stat_far,
    p_sem, vis_sem, gain_sem, q_sem, w_sem, t_sem,
    v_send, v_recv, vm_send, vm_recv, wt_send, wt_recv, n_send, n_recv, o_send, o_recv,
    mt_send, mt_recv, mi_send, mi_recv, ft_send, ft_recv, fi_send, fi_recv,
    s_send, s_recv, z_send, z_recv, up_sem, down_sem,
):
    me, member = lax.axis_index("dp"), lax.axis_index("mp")
    depth = shards // SIDE
    chips = groups // CORES
    y, core = member // CORES, member % CORES
    mate = y * CORES + 1 - core
    z, x = me // SIDE, me % SIDE
    bc = wv.shape[1]
    span = bc // shards
    fold = bc // LANES
    shard_k = wt.shape[1] // shards
    image_rows = q_image.shape[0]
    per_image = image_rows // groups
    text_rows = tv.shape[0]
    rows_dev = per_image + text_rows
    width = groups * bc
    f32, bf16 = jnp.float32, jnp.bfloat16

    far = [lax.rem(y + step, chips) for step in range(1, chips)]
    order = [yy * CORES + lax.rem(core + flip, CORES) for yy in far + [y] for flip in (1, 0)]
    early = len(order) - CORES
    offsets = list(range(1, depth)) + [0]
    targets = [
        lax.rem(z + o, depth) * SIDE + (x if flip else 1 - x) for o in offsets for flip in (0, 1)
    ]
    last = shards - 1

    barrier = pltpu.get_barrier_semaphore()
    across = z * SIDE + 1 - x
    beside = [(me, lax.rem(member + step, groups)) for step in range(1, groups)]
    beside += [(across, lax.rem(member + step, groups)) for step in range(groups)]
    greeted = beside[: groups - 1] + [(across, member)]
    for device in greeted:
        pl.semaphore_signal(barrier, inc=1, device_id=device, device_id_type=MESH)

    @pl.when(z > 0)
    def _():
        pl.semaphore_signal(barrier, inc=1, device_id=(me - SIDE, member), device_id_type=MESH)

    @pl.when(z < depth - 1)
    def _():
        pl.semaphore_signal(barrier, inc=1, device_id=(me + SIDE, member), device_id_type=MESH)

    own_rows = pl.ds(pl.multiple_of(me * image_rows, image_rows), image_rows)
    vis_copy = pltpu.make_async_copy(vision_hbm, vv.at[own_rows], vis_sem)
    vis_copy.start()
    p_copy = pltpu.make_async_copy(proj_hbm, pv, p_sem)
    p_copy.start()
    q_copies = [
        pltpu.make_async_copy(
            q_hbm.at[pl.ds(g * rows_dev + first, count)], dst.at[pl.ds(g * count, count)], q_sem.at[k]
        )
        for k, (first, count, dst) in enumerate(((0, per_image, q_image), (per_image, text_rows, q_text)))
        for g in range(groups)
    ]
    q_image_done = pltpu.make_async_copy(q_hbm.at[pl.ds(0, image_rows)], q_image, q_sem.at[0])
    q_text_done = pltpu.make_async_copy(q_hbm.at[pl.ds(0, groups * text_rows)], q_text, q_sem.at[1])
    w_copies = [pltpu.make_async_copy(w_hbm.at[j], wv.at[j], w_sem.at[k]) for k, j in enumerate(order)]
    gain_copy = pltpu.make_async_copy(gain_hbm, gain_ref, gain_sem)
    t_copy = pltpu.make_async_copy(text_hbm, tv, t_sem)
    for copy in q_copies[:groups] + w_copies[:1]:
        copy.start()

    def pass_on(hop):
        @pl.when(z == hop)
        def _():
            if hop > 0:
                pl.semaphore_wait(up_sem, 1)
            if hop < depth - 1:
                pl.semaphore_signal(up_sem, inc=1, device_id=(me + SIDE, member), device_id_type=MESH)

        @pl.when(depth - 1 - z == hop)
        def _():
            if hop > 0:
                pl.semaphore_wait(down_sem, 1)
            if hop < depth - 1:
                pl.semaphore_signal(down_sem, inc=1, device_id=(me - SIDE, member), device_id_type=MESH)

    vis_copy.wait()
    for copy in w_copies[1:] + q_copies[groups:] + [gain_copy, t_copy]:
        copy.start()

    @pl.when((z == 0) | (z == depth - 1))
    def _():
        pl.semaphore_wait(barrier, len(greeted) + 1)

    @pl.when((z > 0) & (z < depth - 1))
    def _():
        pl.semaphore_wait(barrier, len(greeted) + 2)

    vision = VisionGather(depth, me, member, vv, image_rows, v_send, v_recv, vm_send, vm_recv)
    vision.start()
    pass_on(0)

    p_copy.wait()
    w_flat[...] = pv[...].astype(f32)
    for j in range(shards):
        w_out[j] = w_flat[pl.ds(j, shard_k, stride=fold), :].astype(bf16).T
    own_k = pl.ds(pl.multiple_of(me * shard_k, shard_k), shard_k)
    wt[:, own_k] = w_out[me]

    def w_to(t):
        j = targets[t]
        return remote(w_out.at[j], wt.at[:, own_k], wt_send, wt_recv, (j, member))

    def all_to(buf, send, recv):
        place = buf.at[pl.ds(0, last)]
        return remote(place, place, send, recv, (me, mate))

    def send_w(stage):
        for t in range(last):
            level = targets[t] // SIDE
            outward = jnp.where(z < depth // 2, z + 1, z - 1)
            straight = (level == z) | ((level - z) * (level - z) == 1) & (targets[t] % SIDE == x)
            aside = jnp.logical_not(straight) & (level == outward)
            due = (straight, aside, jnp.logical_not(straight | aside))[stage]

            @pl.when(due)
            def _():
                w_to(t).start()

    send_w(0)

    def text_to_mate(k):
        j = order[k]
        return remote(own_text.at[j, 1 - core], mate_text.at[j], mt_send, mt_recv.at[j], (me, mate))

    def image_to_mate(yy):
        return remote(
            own_image.at[yy * CORES + 1 - core], mate_image.at[yy],
            mi_send, mi_recv.at[yy], (me, mate),
        )

    def text_to_far(k, yy):
        j = order[k]
        return remote(
            sum_text.at[j, yy], far_text.at[y, j], ft_send, ft_recv, (me, yy * CORES + core)
        )

    def piece(t):
        return pl.ds(pl.multiple_of(targets[t] * span, span), span)

    def image_to_far(yy, t):
        return remote(
            sum_image.at[yy, piece(t)], far_image.at[y, piece(t)],
            fi_send, fi_recv.at[t], (me, yy * CORES + core),
        )

    def image_from_far(yy, t):
        return remote(
            sum_image.at[yy, piece(t)], far_image.at[yy, piece(t)],
            fi_send, fi_recv.at[t], (me, yy * CORES + core),
        )

    def image_multiply(k):
        j = order[k]
        w_copies[k].wait()

        @pl.loop(0, bc // TILE)
        def _(n):
            rows = pl.ds(pl.multiple_of(n * TILE, TILE), TILE)
            own_image[j, rows] = row_term(wv[j, rows], q_image[...]).astype(bf16)

        if k % CORES == 0:
            image_to_mate((far + [y])[k // CORES]).start()

    def text_multiply(k, part, parts):
        j = order[k]
        cols = slice(part * bc // parts, (part + 1) * bc // parts)
        term = row_term(q_text[...], wv[j, cols]).astype(bf16)
        for g in range(groups):
            own_text[j, g % CORES, g // CORES, :, cols] = term[g * text_rows : (g + 1) * text_rows]
        if part == parts - 1:
            text_to_mate(k).start()

    def add_image(yy):
        image_to_mate(yy).wait_recv()
        for t in range(shards):
            rows = piece(t)
            total = own_image[yy * CORES + core, rows].astype(f32) + mate_image[yy, rows].astype(f32)
            sum_image[yy, rows] = total.astype(bf16)
            image_to_far(yy, t).start()

    def add_text(k):
        j = order[k]
        text_to_mate(k).wait_recv()
        for yy in far:
            @pl.loop(0, text_rows // ROW_STEP)
            def _(n):
                rows = pl.ds(pl.multiple_of(n * ROW_STEP, ROW_STEP), ROW_STEP)
                total = own_text[j, core, yy, rows].astype(f32) + mate_text[j, yy, rows].astype(f32)
                sum_text[j, yy, rows] = total.astype(bf16)
            text_to_far(k, yy).start()

    lanes = lax.broadcasted_iota(jnp.int32, (span, image_rows), 1)
    slots = lax.rem(lanes, per_image)
    held = jnp.zeros((span, image_rows), jnp.int32)
    for g in range(groups):
        held = jnp.where(lanes // per_image == g, count_ref[g] * PATCH, held)
    live = slots < held

    def n_to(t):
        j = targets[t]
        return remote(n_out.at[t], nt.at[:, own_lanes], n_send, n_recv, (j, member))

    own_lanes = pl.ds(pl.multiple_of(me * image_rows, image_rows), image_rows)

    def spread_image(t):
        if t == 0:
            image_to_mate(y).wait_recv()
        for yy in far:
            image_from_far(yy, t).wait_recv()
        rows = piece(t)
        total = own_image[member, rows].astype(f32) + mate_image[y, rows].astype(f32)
        for yy in far:
            total = total + far_image[yy, rows].astype(f32)
        total = jnp.where(live, total, 0.0).astype(bf16)
        if t < last:
            n_out[t] = total
            n_to(t).start()
        else:
            nt[:, own_lanes] = total

    def each(action, *lead):
        return [functools.partial(action, *lead, chunk) for chunk in range(CHUNKS)]

    def play(*actions):
        for action in actions:
            action()

    images = [functools.partial(spread_image, t) for t in range(shards)]

    def part(k, h):
        return functools.partial(text_multiply, k, h, 2)

    hops = [None] + [each(vision.relay, hop) for hop in range(1, depth)]
    sides = [each(vision.side, hop) for hop in range(depth)]

    q_image_done.wait()
    for k in range(len(order)):
        image_multiply(k)
        if k + 1 < depth - 1:
            pass_on(k + 1)
        if k % CORES == 0 and k >= CORES:
            add_image(far[k // CORES - 1])
            if k == CORES:
                play(*hops[1][:1])
    for hop in range(min(len(order) + 1, depth - 1), depth):
        pass_on(hop)
    q_text_done.wait()
    play(hops[1][1], part(0, 0), hops[1][2], part(0, 1), *hops[1][3:])
    send_w(1)
    play(*sides[0])
    play(hops[2][0], part(1, 0), *hops[2][1:3], part(1, 1), *hops[2][3:])
    send_w(2)
    play(*images[:4])
    add_text(0)
    add_text(1)
    play(part(2, 0), *images[4:6], part(2, 1), *images[6:], *sides[1], part(3, 0), part(3, 1))
    for k in range(4, len(order)):
        play(part(k, 0), part(k, 1))
    gain_copy.wait()
    own_gain = gain_ref[:, pl.ds(pl.multiple_of(member * bc + me * span, span), span)]
    gain_t[...] = jnp.broadcast_to(own_gain, (image_rows, span)).T
    for hop in range(3, depth):
        for chunk in range(CHUNKS):
            play(hops[hop][chunk], sides[hop - 1][chunk])
    all_to(w_out, wt_send, wt_recv).wait_recv()

    def embed(zz):
        vision.arrive(zz)
        pair = pl.ds(pl.multiple_of(zz * SIDE * image_rows, SIDE * image_rows), SIDE * image_rows)
        rounded = row_term(wt[...], vv[pair]).astype(bf16)
        xt[:, pair] = rounded
        value = rounded.astype(f32)
        squares = jnp.sum(value * value, axis=0, keepdims=True)
        for s in range(SIDE):
            stat_f32[pl.ds(zz * SIDE + s, 1)] = squares[:, s * image_rows : (s + 1) * image_rows]

    for hop in range(depth - 2):
        vision.levels(hop, embed)
    play(*sides[depth - 1])
    for hop in range(depth - 2, depth):
        vision.levels(hop, embed)

    all_to(n_out, n_send, n_recv).wait_recv()
    for j in range(shards):
        cols = pl.ds(j * image_rows, image_rows)
        scaled = gain_t[...] * nt[:, cols].astype(f32)
        inner = jnp.sum(scaled * xt[:, cols].astype(f32), axis=0, keepdims=True)
        stat_f32[pl.ds(shards + j, 1)] = inner
    stat_own[...] = stat_f32[...].astype(bf16)

    def stat_to(k):
        device = beside[k]
        mine = lax.rem(me, SIDE) * groups + member
        return remote(stat_own, stat_near.at[mine], s_send, s_recv, device)

    near_done = pl.ds(0, len(beside))
    stat_near_done = remote(
        stat_near.at[near_done], stat_near.at[near_done], s_send, s_recv, (me, mate)
    )
    for k in range(len(beside)):
        stat_to(k).start()
    for k in range(2, len(order)):
        add_text(k)
    total = stat_f32[...]
    stat_near_done.wait_recv()
    for device in beside:
        total = total + stat_near[lax.rem(device[0], SIDE) * groups + device[1]].astype(f32)
    stat_sum[...] = total.astype(bf16)

    def line_to(o):
        target = lax.rem(z + o, depth)
        return remote(stat_sum, stat_far.at[z], z_send, z_recv, (target * SIDE + x, member))

    far_done = pl.ds(0, depth - 1)
    stat_far_done = remote(
        stat_far.at[far_done], stat_far.at[far_done], z_send, z_recv, (me, mate)
    )
    for o in range(1, depth):
        line_to(o).start()
    stat_far_done.wait_recv()
    for o in range(1, depth):
        total = total + stat_far[lax.rem(z + o, depth)].astype(f32)

    inv_all = lax.rsqrt(total[:shards] / width + norm_eps)
    pull_all = inv_all**3 * (total[shards:] / width)
    for b in range(shards):
        cols = pl.ds(b * image_rows, image_rows)
        scaled = gain_t[...] * nt[:, cols].astype(f32)
        grad = inv_all[b : b + 1] * scaled - xt[:, cols].astype(f32) * pull_all[b : b + 1]
        gt[:, cols] = grad.astype(bf16)

    def o_to(t):
        j = targets[t]
        return remote(o_out.at[j], o_in.at[me], o_send, o_recv.at[me], (j, member))

    def o_from(t):
        j = targets[t]
        return remote(o_out.at[j], o_in.at[j], o_send, o_recv.at[j], (j, member))

    out = (jnp.dot(gt[...], vv[...], preferred_element_type=f32) * grad_scale).astype(bf16)
    for j in range(shards):
        o_out[j] = out[:, j * shard_k : (j + 1) * shard_k]
    for t in range(last):
        o_to(t).start()

    text_far = sum_text.at[:, pl.ds(0, len(far))]
    text_far_done = remote(text_far, text_far, ft_send, ft_recv, (me, mate))
    text_far_done.wait_recv()
    t_copy.wait()

    @pl.loop(0, text_rows // ROW_STEP)
    def _(n):
        rows = pl.ds(pl.multiple_of(n * ROW_STEP, ROW_STEP), ROW_STEP)
        squares = jnp.zeros((ROW_STEP, 1), f32)
        inner = jnp.zeros((ROW_STEP, 1), f32)
        for j in range(groups):
            cols = pl.ds(j * bc, bc)
            x = tv[rows, cols].astype(f32)
            norm = own_text[j, core, y, rows].astype(f32) + mate_text[j, y, rows].astype(f32)
            for yy in far:
                norm = norm + far_text[yy, j, rows].astype(f32)
            scaled = gain_ref[:, cols] * norm
            squares += jnp.sum(x * x, axis=1, keepdims=True)
            inner += jnp.sum(x * scaled, axis=1, keepdims=True)
        inv = lax.rsqrt(squares / width + norm_eps)
        pull = inv**3 * (inner / width)
        for j in range(groups):
            cols = pl.ds(j * bc, bc)
            x = tv[rows, cols].astype(f32)
            norm = own_text[j, core, y, rows].astype(f32) + mate_text[j, y, rows].astype(f32)
            for yy in far:
                norm = norm + far_text[yy, j, rows].astype(f32)
            text_out[rows, cols] = (inv * (gain_ref[:, cols] * norm) - x * pull).astype(bf16)

    def finish(chunk, j):
        proj_out[pl.ds(j, shard_k, stride=fold), :] = chunk.astype(f32).T

    finish(o_out[me], me)
    for t in reversed(range(last)):
        o_from(t).wait_recv()
        finish(o_in[targets[t]], targets[t])

    vision.drain()
    all_to(w_out, wt_send, wt_recv).wait_send()
    all_to(n_out, n_send, n_recv).wait_send()
    all_to(o_out, o_send, o_recv.at[0]).wait_send()
    stat_near_done.wait_send()
    stat_far_done.wait_send()
    text_far_done.wait_send()
    remote(mate_text, mate_text, mt_send, mt_recv.at[0], (me, mate)).wait_send()
    remote(mate_image, mate_image, mi_send, mi_recv.at[0], (me, mate)).wait_send()
    image_far = sum_image.at[pl.ds(0, len(far))]
    remote(image_far, image_far, fi_send, fi_recv.at[0], (me, mate)).wait_send()


def place_outputs(text_in, proj_in, text_out, proj_out, sem):
    copies = []
    for k, (src, dst) in enumerate(((text_in, text_out), (proj_in, proj_out))):
        step = src.shape[0] // PIECES
        for p in range(PIECES):
            rows = pl.ds(p * step, step)
            copies.append(pltpu.make_async_copy(src.at[rows], dst.at[rows], sem.at[k, p]))
    for copy in copies:
        copy.start()
    for copy in copies:
        copy.wait()


def live_rows(image_count, groups):
    image_rows = IMG_MAX * PATCH
    row_ids = jnp.arange(groups * image_rows, dtype=jnp.int32)
    owners = row_ids // image_rows
    slot_ids = row_ids % image_rows // PATCH
    owner_match = owners[:, None] == jnp.arange(groups, dtype=jnp.int32)[None, :]
    owner_counts = jnp.sum(jnp.where(owner_match, image_count[None, :], 0), axis=1)
    return (slot_ids < owner_counts)[:, None]


def fused_body(vision_rows, image_count, proj_flat, text_embeds, norm_gain, q_weight, q_grad):
    groups, shards = lax.axis_size("mp"), lax.axis_size("dp")
    model_width, bc = q_weight.shape
    image_rows, enc_width = vision_rows.shape
    text_rows = text_embeds.shape[0]
    shard_k = proj_flat.shape[0] * proj_flat.shape[1] // bc
    span = bc // shards
    chips, depth = groups // CORES, shards // SIDE
    all_rows = shards * image_rows
    grad_scale = 1.0 / float(all_rows) ** 0.5
    f32, bf16 = jnp.float32, jnp.bfloat16
    vmem, dma = pltpu.VMEM, pltpu.SemaphoreType.DMA
    on_chip = pl.BlockSpec(memory_space=pltpu.VMEM)
    scalars = pl.BlockSpec(memory_space=pltpu.SMEM)
    in_hbm = pl.BlockSpec(memory_space=pltpu.HBM)
    text_grad, proj_block = pl.pallas_call(
        functools.partial(kernel, shards, groups, grad_scale),
        name="projector_backward",
        out_shape=(vmem(text_embeds.shape, bf16), vmem(proj_flat.shape, f32)),
        in_specs=[scalars] + [in_hbm] * 6,
        out_specs=(on_chip, on_chip),
        scratch_shapes=[
            vmem(proj_flat.shape, bf16),
            vmem((all_rows, enc_width), bf16),
            vmem((1, model_width), f32),
            vmem((image_rows, bc), bf16),
            vmem((groups * text_rows, bc), bf16),
            vmem((groups, bc, bc), bf16),
            vmem(text_embeds.shape, bf16),
            vmem((groups, CORES, chips, text_rows, bc), bf16),
            vmem((groups, bc, image_rows), bf16),
            vmem((groups, chips, text_rows, bc), bf16),
            vmem((chips, bc, image_rows), bf16),
            vmem((groups, chips, text_rows, bc), bf16),
            vmem((chips, bc, image_rows), bf16),
            vmem((chips, groups, text_rows, bc), bf16),
            vmem((chips, bc, image_rows), bf16),
            vmem(proj_flat.shape, f32),
            vmem((shards, span, shard_k), bf16),
            vmem((span, enc_width), bf16),
            vmem((shards, span, image_rows), bf16),
            vmem((span, all_rows), bf16),
            vmem((span, all_rows), bf16),
            vmem((span, all_rows), bf16),
            vmem((span, image_rows), f32),
            vmem((shards, span, shard_k), bf16),
            vmem((shards, span, shard_k), bf16),
            vmem((2 * shards, image_rows), f32),
            vmem((2 * shards, image_rows), bf16),
            vmem((SIDE * groups, 2 * shards, image_rows), bf16),
            vmem((2 * shards, image_rows), bf16),
            vmem((depth, 2 * shards, image_rows), bf16),
            dma, dma, dma, dma((2,)), dma((groups,)), dma,
            dma((3,)), dma((shards, CHUNKS)), dma, dma((shards,)),
            dma, dma, dma, dma, dma, dma((shards,)),
            dma, dma((groups,)), dma, dma((chips,)), dma, dma, dma, dma((shards,)),
            dma, dma, dma, dma, pltpu.SemaphoreType.REGULAR, pltpu.SemaphoreType.REGULAR,
        ],
        compiler_params=pltpu.CompilerParams(
            collective_id=0, has_side_effects=True, vmem_limit_bytes=56 * 1024 * 1024
        ),
    )(
        image_count,
        proj_flat,
        vision_rows,
        norm_gain[None, :],
        q_grad,
        q_weight.reshape(groups, bc, bc),
        text_embeds,
    )
    kinds = (text_grad, proj_block)
    return pl.pallas_call(
        place_outputs,
        name="place_outputs",
        out_shape=tuple(jax.ShapeDtypeStruct(a.shape, a.dtype) for a in kinds),
        in_specs=[on_chip] * 2,
        out_specs=(in_hbm, in_hbm),
        scratch_shapes=[dma((2, PIECES))],
        compiler_params=pltpu.CompilerParams(vmem_limit_bytes=4 * 1024 * 1024),
    )(*kinds)


def norm_back(rows_in, grads, gain):
    inputs = rows_in.astype(jnp.float32)
    inv_rms = lax.rsqrt(jnp.mean(inputs * inputs, axis=-1, keepdims=True) + norm_eps)
    scaled = gain[None, :] * grads
    inner_mean = jnp.mean(scaled * inputs, axis=-1, keepdims=True)
    return inv_rms * scaled - inputs * inv_rms**3 * inner_mean


def general_body(vision_rows, image_count, proj_flat, text_embeds, norm_gain, q_weight, q_grad):
    groups = lax.axis_size("mp")
    member = lax.axis_index("mp")
    shards = lax.axis_size("dp")
    enc_width = vision_rows.shape[1]
    block_cols = q_weight.shape[1]
    model_width = q_weight.shape[0]
    used_count = enc_width * block_cols
    image_rows = IMG_MAX * PATCH
    gathered = lax.all_gather(proj_flat, "dp", axis=0, tiled=True)
    proj_block = gathered.reshape(-1)[:used_count].reshape(enc_width, block_cols)
    embed_cols = jnp.dot(vision_rows, proj_block, preferred_element_type=jnp.float32).astype(
        jnp.bfloat16
    )
    live_group = live_rows(image_count, groups)
    blocks = q_grad.reshape(groups, ROWS_DEV, block_cols)
    image_query = blocks[:, :image_rows].reshape(-1, block_cols)
    text_query = blocks[:, image_rows:].reshape(-1, block_cols)
    image_term = row_term(image_query, q_weight)
    image_norm = lax.psum_scatter(
        image_term.astype(jnp.bfloat16), "mp", scatter_dimension=1, tiled=True
    ).astype(jnp.float32)
    text_norm = lax.psum_scatter(
        row_term(text_query, q_weight).astype(jnp.bfloat16), "mp", scatter_dimension=0, tiled=True
    ).astype(jnp.float32)
    x_cols = embed_cols.astype(jnp.float32)
    gain_cols = lax.dynamic_slice_in_dim(norm_gain, member * block_cols, block_cols)
    scaled = gain_cols[None, :] * image_norm
    squares, inner_sum = lax.psum(
        (jnp.sum(x_cols * x_cols, axis=1), jnp.sum(scaled * x_cols, axis=1)), "mp"
    )
    inv_rms = lax.rsqrt(squares / model_width + norm_eps)[:, None]
    image_input = inv_rms * scaled - x_cols * inv_rms**3 * (inner_sum / model_width)[:, None]
    image_cols = jnp.where(live_group, image_input, 0.0).astype(jnp.bfloat16)
    text_grad = norm_back(text_embeds, text_norm, norm_gain).astype(jnp.bfloat16)
    grad_scale = 1.0 / jnp.sqrt(jnp.float32(shards * groups * image_rows))
    proj_part = (
        lax.dot_general(
            vision_rows, image_cols, (((0,), (0,)), ((), ())), preferred_element_type=jnp.float32
        )
        * grad_scale
    )
    stored_rows = proj_flat.shape[0]
    padded = jnp.pad(proj_part.reshape(-1), (0, shards * stored_rows * 128 - used_count))
    padded = padded.reshape(shards * stored_rows, 128)
    proj_grad = lax.psum_scatter(padded, "dp", scatter_dimension=0, tiled=True)
    return (text_grad, proj_grad)


def body(vision_rows, image_count, proj_flat, text_embeds, norm_gain, q_weight, q_grad):
    groups, shards = lax.axis_size("mp"), lax.axis_size("dp")
    bc = q_weight.shape[1]
    count = proj_flat.shape[0] * proj_flat.shape[1]
    shard_k = count // bc
    fits = (
        count % bc == 0
        and shard_k == LANES
        and bc == shards * LANES
        and bc % TILE == 0
        and shard_k * shards == vision_rows.shape[1]
        and shard_k == vision_rows.shape[0]
        and groups == 2 * CORES
        and groups % CORES == 0
        and vision_rows.shape[0] // groups % ROW_STEP == 0
        and text_embeds.shape[0] % (PIECES * ROW_STEP) == 0
        and shards > 2 * SIDE
        and shards % SIDE == 0
    )
    run = fused_body if fits else general_body
    return run(vision_rows, image_count, proj_flat, text_embeds, norm_gain, q_weight, q_grad)


def solution(mesh):
    return jax.shard_map(
        body,
        mesh=mesh,
        in_specs=(
            P("dp", None),
            P("dp"),
            P(("dp", "mp"), None),
            P(("dp", "mp"), None),
            P(),
            P(None, "mp"),
            P("dp", "mp"),
        ),
        out_specs=(P(("dp", "mp"), None), P(("dp", "mp"), None)),
        check_vma=False,
    )
```
